512 devices in a mesh: groups: 2 (over y), trades: 32 (over z), scen: 4 (over x), fact: 2 (over core).
Axes of the slice: x: 4, y: 2, z: 32, core: 2. Of those that a mesh axis runs over, the one named last changes fastest.
The devices are a block of a 4x8x32 slice.
Arguments:
- scenario_state: bfloat16 [256, 256], P(('groups', 'scen')), parts along dimension 0, may hold values from -6 to 6
- direction: bfloat16 [16384, 256], P('trades'), may hold values from -0.375 to 0.375
- trade_load: bfloat16 [16384, 256], P('trades', 'fact'), may hold values from -6 to 6
- trade_curve: bfloat16 [16384, 256], P('trades', 'fact'), may hold values from -3 to 3
- trade_set: int32 [16384], P('trades'), may hold values from 0 to 127, as said below
- factor_bucket_index: int32 [256], P('fact'), may hold values from 0 to 11
- threshold: float32 [12], replicated, may hold values from 5 to 500
- factor_risk_weight: float32 [256], P('fact'), may hold values from 0.5 to 2
- correlation: float32 [256, 256], P(None, 'fact'), may hold values from -1 to 1, as said below
- funding: float32 [256, 128], P(('groups', 'scen')), parts along dimension 0, may hold values from 0.05 to 0.5
Outputs:
- state_grad: float32 [256, 256], P(('groups', 'scen'), 'fact'), parts along dimension 0
- weight_grad: float32 [512], P(('groups', 'fact')), parts along dimension 0
The draws below stay inside these ranges and needn't reach their ends.
There are 2 independent parts, one for each index of `groups`. The reference program is written for one: setup_inputs(seed, part) draws one part's arguments, and reference() takes and returns one part's arrays. A program takes and returns all parts, laid end to end along the dimension named above; an argument that names none is the same for every part. Nothing has to cross between parts.
Inputs may be any that keep to these rules, and one draw needn't show every extreme that they name: `trade_set`: never falling along the trades; set 0 begins at trade 0, and set n begins at a trade of n * 128 to (n + 1) * 128 - 1. `correlation`: symmetric positive definite with unit diagonal.
All inputs are finite; a program needn't handle non-finite values.
Results may differ from the reference program's by a relative error of at most 0.009.
Values may be sent and summed in bfloat16 or wider, within the bound.
No kernel may reach another device: no remote copies, remote signals or barrier semaphores. Data moves between devices by JAX's collectives and lax.ppermute only.
A program may use at most 64 MiB of HBM per device.

```python
import math
import jax
import jax.numpy as jnp
from jax import lax

K = 256
NBUCK = 12
TRADES = 16384
SCEN = 128
NSETS = 128


def draw_correlation(key, part):
    base = jax.random.normal(jax.random.fold_in(key, 11), (K, K), jnp.float32)
    shaped = jnp.dot(base, base.T, precision=lax.Precision.HIGHEST) / K + 0.5 * jnp.eye(K, dtype=jnp.float32)
    scaling = 1.0 / jnp.sqrt(jnp.diagonal(shaped))
    return shaped * scaling[:, None] * scaling[None, :]


def draw_trade_set(key, part):
    spacing = TRADES // NSETS
    jitter = jax.random.randint(jax.random.fold_in(key, 5), (NSETS,), 0, spacing, dtype=jnp.int32)
    order = jnp.arange(NSETS, dtype=jnp.int32)
    jitter = jnp.where(order == 0, jnp.int32(0), jitter)
    starts = order * spacing + jitter
    position = jnp.arange(TRADES, dtype=jnp.int32)
    begun = (position[:, None] >= starts[None, :]).astype(jnp.int32)
    return (jnp.sum(begun, axis=1) - 1).astype(jnp.int32)


def set_ends(values, rng, low, largest):
    longest = values.shape.index(max(values.shape))
    spots = []
    for shift in (0, 1):
        where = [jax.random.randint(jax.random.fold_in(rng, axis), (), 0, length) for axis, length in enumerate(values.shape)]
        where[longest] = (where[longest] + shift) % values.shape[longest]
        spots.append(tuple(where))
    return values.at[spots[0]].set(low).at[spots[1]].set(largest)


def steps_of(own_key, shape, split, low, top_value):
    def one(axis_at, shards_of):
        heights = jax.random.uniform(jax.random.fold_in(jax.random.fold_in(own_key, 6), axis_at), (shards_of,), jnp.float32, low / len(split), top_value / len(split))
        return jnp.repeat(jnp.exp(heights), shape[axis_at] // shards_of).reshape((-1,) + (1,) * (len(shape) - axis_at - 1))

    loudness = one(*split[0])
    for cut in split[1:]:
        loudness = loudness * one(*cut)
    return loudness


def normal_values(own_key, extent, width, reach, pieces=(), kind=jnp.bfloat16):
    result = jax.random.normal(own_key, extent, jnp.float32) * width
    if len(pieces) > 0:
        result = steps_of(own_key, extent, pieces, -0.22, 0.18) * result
    return jnp.clip(result, min=-reach, max=reach).astype(kind)


def setup_inputs(seed: int = 0, part: int = 0) -> dict:
    splits = jax.random.split(jax.random.key(seed), 11)
    own_keys = jax.random.split(jax.random.fold_in(splits[10], part), 11)
    scenario_state = normal_values(own_keys[0], (SCEN, K), 1.0, 6.0, ((0, 4),))
    direction = normal_values(splits[1], (TRADES, K), K ** -0.5, 0.375, ((0, 32),))
    trade_load = normal_values(splits[2], (TRADES, K), 1.0, 6.0, ((0, 32), (1, 2)))
    trade_curve = normal_values(splits[3], (TRADES, K), 0.5, 3.0, ((0, 32), (1, 2)))
    trade_set = draw_trade_set(jax.random.fold_in(splits[10], 71), part)
    factor_bucket_index = set_ends(jax.random.randint(splits[5], (K,), 0, NBUCK), jax.random.fold_in(splits[5], 1), 0, NBUCK - 1).astype(jnp.int32)
    threshold = jnp.clip(jnp.exp(jax.random.uniform(splits[6], (NBUCK,), jnp.float32, math.log(5.0), math.log(500.0))), 5.0, 500.0)
    factor_risk_weight = jnp.clip(jnp.exp(math.log(2.0) - 1.3862944 * jax.random.uniform(splits[7], (K,), jnp.float32) ** steps_of(splits[7], (K,), ((0, 2),), -0.2, 0.2)), 0.5, 2.0)
    correlation = draw_correlation(jax.random.fold_in(splits[10], 71), part)
    funding = jnp.clip(jnp.exp(math.log(0.5) - 2.3025851 * jax.random.uniform(own_keys[9], (SCEN, NSETS), jnp.float32) ** steps_of(own_keys[9], (SCEN, NSETS), ((0, 4),), -0.2, 0.2)), 0.05, 0.5)
    return {"scenario_state": scenario_state, "direction": direction, "trade_load": trade_load, "trade_curve": trade_curve, "trade_set": trade_set, "factor_bucket_index": factor_bucket_index, "threshold": threshold, "factor_risk_weight": factor_risk_weight, "correlation": correlation, "funding": funding}


def reference(scenario_state, direction, trade_load, trade_curve, trade_set, factor_bucket_index, threshold, factor_risk_weight, correlation, funding):
    precise = lax.Precision.HIGHEST
    moneyness = jnp.dot(scenario_state, direction.T, preferred_element_type=jnp.float32)
    likely = jax.nn.sigmoid(moneyness)
    likely_round = likely.astype(jnp.bfloat16)
    money_round = moneyness.astype(jnp.bfloat16)
    load_full = trade_load.astype(jnp.float32)
    curve_full = trade_curve.astype(jnp.float32)

    def one_net(scen_row):
        likely_row, money_row = scen_row
        terms = likely_row.astype(jnp.float32)[:, None] * load_full + money_row.astype(jnp.float32)[:, None] * curve_full
        return jax.ops.segment_sum(terms, trade_set, num_segments=NSETS)
    netted_sensitivity = lax.map(one_net, (likely_round, money_round))
    bucket_hot = (factor_bucket_index[:, None] == jnp.arange(NBUCK, dtype=jnp.int32)[None, :]).astype(jnp.float32)
    bucket_sum = jnp.einsum('snk,kb->snb', netted_sensitivity, bucket_hot, precision=precise)
    raw_ratio = jnp.sqrt(jnp.abs(bucket_sum) / threshold)
    concentration = jnp.maximum(jnp.float32(1.0), raw_ratio)
    conc_factor = concentration[..., factor_bucket_index]
    weighted = factor_risk_weight * netted_sensitivity * conc_factor
    corr_image = jnp.einsum('snl,kl->snk', weighted, correlation, precision=precise)
    margin = jnp.sqrt(lax.optimization_barrier(jnp.sum(weighted * corr_image, -1)) + 1e-06)
    weighted_bar = (funding / margin)[..., None] * corr_image
    conc_bar = jnp.einsum('snk,kb->snb', weighted_bar * factor_risk_weight * netted_sensitivity, bucket_hot, precision=precise)
    bucket_bar = jnp.where(raw_ratio > 1.0, conc_bar * jnp.sign(bucket_sum) / (2.0 * threshold * concentration), jnp.float32(0.0))
    netted_sensitivity_bar = (weighted_bar * factor_risk_weight * conc_factor + bucket_bar[..., factor_bucket_index]).astype(jnp.bfloat16)
    weight_grad = lax.optimization_barrier(jnp.sum(weighted_bar * netted_sensitivity * conc_factor, axis=(0, 1))) / (SCEN * NSETS)

    def one_back(scen_row):
        pulled = scen_row[0][trade_set].astype(jnp.float32)
        return (lax.optimization_barrier(jnp.sum(pulled * load_full, -1)), lax.optimization_barrier(jnp.sum(pulled * curve_full, -1)))
    load_pull, curve_pull = lax.map(one_back, (netted_sensitivity_bar,))
    money_bar = (load_pull * likely * (1.0 - likely) + curve_pull).astype(jnp.bfloat16)
    state_grad = jnp.dot(money_bar, direction, preferred_element_type=jnp.float32)
    return (state_grad, weight_grad)
```

```python
import jax
import jax.numpy as jnp
from jax import lax
from jax.experimental import pallas as pl
from jax.experimental.pallas import tpu as pltpu
from jax.sharding import PartitionSpec as P

NSET_DEV = 4
SPAN = NSET_DEV + 1
NEAR = 4
F32 = jnp.float32
BF16 = jnp.bfloat16
PRECISE = lax.Precision.HIGHEST


def three_parts(x):
    high = x.astype(BF16)
    rest = x - high.astype(F32)
    mid = rest.astype(BF16)
    low = (rest - mid.astype(F32)).astype(BF16)
    return high, mid, low


def from_parts(high, mid, low):
    return high.astype(F32) + mid.astype(F32) + low.astype(F32)


def dot_t(a, b, **kw):
    return lax.dot_general(a, b, (((1,), (1,)), ((), ())), preferred_element_type=F32, **kw)


def dot(a, b, **kw):
    return lax.dot_general(a, b, (((1,), (0,)), ((), ())), preferred_element_type=F32, **kw)


def pack_kernel(load, curve, corr, small, out):
    trades, half = load.shape
    start = pl.multiple_of(lax.axis_index("fact") * half, half)
    out[:trades] = load[...]
    out[trades : 2 * trades] = curve[...]
    parts = three_parts(corr[pl.ds(start, half)])
    for i, part in enumerate(parts):
        out[2 * trades + i * half : 2 * trades + (i + 1) * half] = part
    parts = three_parts(small[...])
    base = 2 * trades + 3 * half
    for i, part in enumerate(parts):
        out[base + 8 * i : base + 8 * (i + 1)] = part


def money_kernel(state, direction, money_out, pair_out):
    money = dot_t(state[...], direction[...])
    money_out[...] = money
    trades = direction.shape[0]
    pair_out[:, :trades] = lax.logistic(money).astype(BF16)
    pair_out[:, trades:] = money.astype(BF16)


def window_kernel(pair, sets, mine, other, net_out):
    scen, double = pair.shape
    trades = double // 2
    first = lax.axis_index("trades") * NSET_DEV - 1
    paired = pair[...]
    where_set = jnp.concatenate([sets[...], sets[...]], axis=1) - first
    half = mine.shape[1]
    own = mine[:double]
    swapped = other[:double]
    for w in range(SPAN):
        member = jnp.where(where_set == w, 1.0, 0.0).astype(BF16)
        mixing = paired * member
        net_out[w * scen : (w + 1) * scen, :half] = dot(mixing, own)
        net_out[w * scen : (w + 1) * scen, half:] = dot(mixing, swapped)


def sets_kernel(
    net, above, below, money, sets, mine, other, corr, threshold, fund, direction,
    state_out, weight_out,
):
    rows, factors = net.shape
    scen = rows // SPAN
    double = 2 * direction.shape[0]
    trades = direction.shape[0]
    half = factors // 2
    side = pl.multiple_of(lax.axis_index("fact") * half, half)
    far_side = pl.multiple_of((1 - lax.axis_index("fact")) * half, half)
    netted = jnp.concatenate(
        [
            net[:scen] + above[...],
            net[scen : (SPAN - 1) * scen],
            net[(SPAN - 1) * scen :] + below[...],
        ],
        axis=0,
    )
    base = double + 3 * half

    def row_of(ref, i):
        return from_parts(ref[base + i : base + i + 1], ref[base + 8 + i : base + 9 + i], ref[base + 16 + i : base + 17 + i])

    risk = jnp.concatenate([row_of(mine, 0), row_of(other, 0)], axis=1)
    bucket = jnp.concatenate([row_of(mine, 1), row_of(other, 1)], axis=1).astype(jnp.int32)
    buckets = threshold.shape[1]
    hot = jnp.where(
        lax.broadcasted_iota(jnp.int32, (buckets, factors), 0) == bucket, 1.0, 0.0
    ).astype(F32)
    limit = threshold[...]
    bucket_sum = dot_t(netted, hot, precision=PRECISE)
    raw_ratio = jnp.sqrt(jnp.abs(bucket_sum) / limit)
    concentration = jnp.maximum(1.0, raw_ratio)
    conc_factor = dot(concentration, hot, precision=PRECISE)
    scaled = risk * conc_factor
    weighted = scaled * netted
    near_cols = corr[pl.ds(side, half)]
    cross = corr[pl.ds(far_side, half)]
    far_cols = from_parts(*[other[double + i * half : double + (i + 1) * half] for i in range(3)])
    w_own, w_far = weighted[:, :half], weighted[:, half:]
    image = jnp.concatenate(
        [
            dot(w_own, near_cols, precision=PRECISE) + dot(w_far, cross, precision=PRECISE),
            dot_t(w_own, cross, precision=PRECISE) + dot(w_far, far_cols, precision=PRECISE),
        ],
        axis=1,
    )
    margin = jnp.sqrt(jnp.sum(weighted * image, axis=1, keepdims=True) + 1e-06)
    weighted_bar = (fund[...] / margin) * image
    conc_bar = dot_t(weighted_bar * risk * netted, hot, precision=PRECISE)
    sign = jnp.where(bucket_sum > 0.0, 1.0, jnp.where(bucket_sum < 0.0, -1.0, 0.0))
    bucket_bar = jnp.where(raw_ratio > 1.0, conc_bar * sign / (2.0 * limit * concentration), 0.0)
    bar = (weighted_bar * scaled + dot(bucket_bar, hot, precision=PRECISE)).astype(BF16)
    grad_terms = weighted_bar[scen:] * netted[scen:] * conc_factor[scen:]
    weight_out[...] = jnp.broadcast_to(jnp.sum(grad_terms[:, :half], axis=0, keepdims=True), weight_out.shape)
    spread = dot_t(bar[:, :half], mine[:double]) + dot_t(bar[:, half:], other[:double])
    first = lax.axis_index("trades") * NSET_DEV - 1
    where_set = jnp.concatenate([sets[...], sets[...]], axis=1) - first
    pulled = jnp.zeros((scen, double), F32)
    for w in range(SPAN):
        pulled = pulled + jnp.where(where_set == w, spread[w * scen : (w + 1) * scen], 0.0)
    likely = lax.logistic(money[...])
    money_bar = (pulled[:, :trades] * likely * (1.0 - likely) + pulled[:, trades:]).astype(BF16)
    state_out[...] = dot(money_bar, direction[:, pl.ds(side, half)])


def call(body, out_shape, *args):
    return pl.pallas_call(
        body,
        out_shape=out_shape,
        in_specs=[pl.BlockSpec(memory_space=pltpu.VMEM)] * len(args),
        out_specs=jax.tree.map(lambda _: pl.BlockSpec(memory_space=pltpu.VMEM), out_shape),
    )(*args)


def shifted(x, axis, by):
    size = lax.axis_size(axis)
    pairs = [(i, i + by) for i in range(size) if 0 <= i + by < size]
    return lax.ppermute(x, axis, pairs)


def exchange(pieces, axes, groups):
    return lax.all_to_all(pieces, axes, 0, 0, tiled=True, axis_index_groups=groups)


def reduce_over_trades(state_part, weight_part):
    devs, cols = lax.axis_size("trades"), lax.axis_size("scen")
    scen, half = state_part.shape
    blocks = devs // NEAR
    rows = scen // NEAR
    near = [
        [(b * NEAR + j) * cols + c for j in range(NEAR) for c in range(cols)]
        for b in range(blocks)
    ]
    pieces = jnp.concatenate(
        [
            state_part.reshape(NEAR, rows * half),
            jnp.broadcast_to(weight_part.reshape(1, half), (NEAR, half)),
        ],
        axis=1,
    ).astype(BF16)
    length = (rows + 1) * half
    pieces = jnp.broadcast_to(pieces[:, None, None], (NEAR, cols, 1, length)).reshape(NEAR * cols, 1, length)
    got = exchange(pieces, ("trades", "scen"), near).reshape(NEAR, cols, length).astype(F32)
    state = lax.dynamic_index_in_dim(got, lax.axis_index("scen"), 1, keepdims=False)
    state = jnp.sum(state[:, : rows * half], axis=0)
    weight = jnp.sum(got[:, :, rows * half :], axis=(0, 1))
    far = [[b * NEAR + j for b in range(blocks)] for j in range(NEAR)]
    piece = jnp.concatenate([state, weight]).astype(BF16)
    pieces = jnp.broadcast_to(piece[None, None], (blocks, 1, length))
    total = jnp.sum(exchange(pieces, "trades", far).reshape(blocks, length).astype(F32), axis=0)
    weight = total[rows * half :]
    group = [[b * NEAR + j for j in range(NEAR)] for b in range(blocks)]
    pieces = jnp.broadcast_to(total[None, None, : rows * half].astype(BF16), (NEAR, 1, rows * half))
    state = exchange(pieces, "trades", group).reshape(scen, half).astype(F32)
    return state, weight


def on_device(
    scenario_state,
    direction,
    trade_load,
    trade_curve,
    trade_set,
    factor_bucket_index,
    threshold,
    factor_risk_weight,
    correlation,
    funding,
):
    scen, set_count = funding.shape
    trades, half = trade_load.shape
    double, factors = 2 * trades, 2 * half
    small = jnp.zeros((8, half), F32)
    small = small.at[0].set(factor_risk_weight).at[1].set(factor_bucket_index.astype(F32))
    mine = call(
        pack_kernel,
        jax.ShapeDtypeStruct((double + 3 * half + 24, half), BF16),
        trade_load, trade_curve, correlation, small,
    )
    other = lax.ppermute(mine, "fact", [(0, 1), (1, 0)])
    money, pair = call(
        money_kernel,
        (jax.ShapeDtypeStruct((scen, trades), F32), jax.ShapeDtypeStruct((scen, double), BF16)),
        scenario_state, direction,
    )
    sets = trade_set.reshape(1, trades)
    net = call(
        window_kernel,
        jax.ShapeDtypeStruct((SPAN * scen, factors), F32),
        pair, sets, mine, other,
    )
    below = shifted(net[:scen], "trades", -1)
    above = shifted(net[(SPAN - 1) * scen :], "trades", 1)
    first = lax.axis_index("trades") * NSET_DEV - 1
    padded = jnp.concatenate([funding[:, :1], funding], axis=1)
    fund = lax.dynamic_slice_in_dim(padded, first + 1, SPAN, 1).T.reshape(SPAN * scen, 1)
    buckets = threshold.shape[0]
    limit = jnp.concatenate([threshold, jnp.ones((-buckets % 16,), F32)]).reshape(1, -1)
    state_part, weight_part = call(
        sets_kernel,
        (jax.ShapeDtypeStruct((scen, half), F32), jax.ShapeDtypeStruct((8, half), F32)),
        net, above, below, money, sets, mine, other, correlation, limit, fund, direction,
    )
    state_grad, weight_sum = reduce_over_trades(state_part, weight_part[:1])
    weight_grad = weight_sum / (scen * lax.axis_size("scen") * set_count)
    return (state_grad, weight_grad)


def solution(mesh):
    placed = (
        P(("groups", "scen"), None),
        P("trades", None),
        P("trades", "fact"),
        P("trades", "fact"),
        P("trades"),
        P("fact"),
        P(),
        P("fact"),
        P(None, "fact"),
        P(("groups", "scen"), None),
    )
    return jax.shard_map(
        on_device,
        mesh=mesh,
        in_specs=placed,
        out_specs=(P(("groups", "scen"), "fact"), P(("groups", "fact"))),
        check_vma=False,
    )
```

```python
import jax
import jax.numpy as jnp
from jax import lax
from jax.experimental import pallas as pl
from jax.experimental.pallas import tpu as pltpu
from jax.sharding import PartitionSpec as P

NSET_DEV = 4
SPAN = NSET_DEV + 1
NEAR = 4
F32 = jnp.float32
BF16 = jnp.bfloat16
PRECISE = lax.Precision.HIGHEST


def three_parts(x):
    high = x.astype(BF16)
    rest = x - high.astype(F32)
    mid = rest.astype(BF16)
    low = (rest - mid.astype(F32)).astype(BF16)
    return high, mid, low


def from_parts(high, mid, low):
    return high.astype(F32) + mid.astype(F32) + low.astype(F32)


def dot_t(a, b, **kw):
    return lax.dot_general(a, b, (((1,), (1,)), ((), ())), preferred_element_type=F32, **kw)


def dot(a, b, **kw):
    return lax.dot_general(a, b, (((1,), (0,)), ((), ())), preferred_element_type=F32, **kw)


def pack_kernel(load, curve, corr, risk, bucket, out):
    trades, half = load.shape
    start = pl.multiple_of(lax.axis_index("fact") * half, half)
    out[:trades] = load[...]
    out[trades : 2 * trades] = curve[...]
    for i, part in enumerate(three_parts(corr[pl.ds(start, half)])):
        out[2 * trades + i * half : 2 * trades + (i + 1) * half] = part
    base = 2 * trades + 3 * half
    high, mid, low = three_parts(risk[...])
    for i, row in enumerate((high, mid, low, bucket[...].astype(F32).astype(BF16))):
        out[base + 8 * i : base + 8 * (i + 1)] = jnp.broadcast_to(row, (8, half))


def money_kernel(
    state, direction, corr, sets, funding, threshold,
    money_out, pair_out, side_out, corr_out, where_out, fund_out, limit_out,
):
    money = dot_t(state[...], direction[...])
    money_out[...] = money
    trades, factors = direction.shape
    half = factors // 2
    pair_out[:, :trades] = lax.logistic(money).astype(BF16)
    pair_out[:, trades:] = money.astype(BF16)
    side = pl.multiple_of(lax.axis_index("fact") * half, half)
    side_out[...] = direction[:, pl.ds(side, half)]
    corr_out[...] = corr[...]
    first = lax.axis_index("trades") * NSET_DEV - 1
    place = jnp.broadcast_to(sets[...] - first, (8, trades))
    where_out[:, :trades] = place
    where_out[:, trades:] = place
    fund_out[...] = funding[...]
    buckets = lax.broadcasted_iota(jnp.int32, limit_out.shape, 1)
    limit = jnp.ones(limit_out.shape, F32)
    for i in range(threshold.shape[0]):
        limit = jnp.where(buckets == i, threshold[i], limit)
    limit_out[...] = limit


def window_kernel(pair, where, mine, other, low_out, mid_out, high_out):
    scen, double = pair.shape
    paired = pair[...]
    place = where[:1]
    half = mine.shape[1]
    for w in range(SPAN):
        member = jnp.where(place == w, 1.0, 0.0).astype(BF16)
        mixing = paired * member
        if w == 0:
            out, at = low_out, 0
        elif w < SPAN - 1:
            out, at = mid_out, (w - 1) * scen
        else:
            out, at = high_out, 0
        out[at : at + scen, :half] = dot(mixing, mine[:double])
        out[at : at + scen, half:] = dot(mixing, other[:double])


def sets_kernel(
    low, mid, high, above, below, mine, other, corr, fund, limits, bar_out, weight_out
):
    scen, factors = low.shape
    half = factors // 2
    double = mine.shape[0] - 3 * half - 32
    side = pl.multiple_of(lax.axis_index("fact") * half, half)
    far_side = pl.multiple_of((1 - lax.axis_index("fact")) * half, half)
    netted = jnp.concatenate([low[...] + above[...], mid[...], high[...] + below[...]], axis=0)
    base = double + 3 * half

    def risk_of(ref):
        return from_parts(ref[base : base + 1], ref[base + 8 : base + 9], ref[base + 16 : base + 17])

    def bucket_of(ref):
        return ref[base + 24 : base + 25].astype(F32)

    risk = jnp.concatenate([risk_of(mine), risk_of(other)], axis=1)
    bucket = jnp.concatenate([bucket_of(mine), bucket_of(other)], axis=1).astype(jnp.int32)
    hot = jnp.where(
        lax.broadcasted_iota(jnp.int32, (16, factors), 0) == bucket, 1.0, 0.0
    ).astype(F32)
    limit = limits[:1, :16]
    bucket_sum = dot_t(netted, hot, precision=PRECISE)
    raw_ratio = jnp.sqrt(jnp.abs(bucket_sum) / limit)
    concentration = jnp.maximum(1.0, raw_ratio)
    conc_factor = dot(concentration, hot, precision=PRECISE)
    scaled = risk * conc_factor
    weighted = scaled * netted
    near_cols = corr[pl.ds(side, half)]
    cross = corr[pl.ds(far_side, half)]
    far_cols = from_parts(*[other[double + i * half : double + (i + 1) * half] for i in range(3)])
    w_own, w_far = weighted[:, :half], weighted[:, half:]
    image = jnp.concatenate(
        [
            dot(w_own, near_cols, precision=PRECISE) + dot(w_far, cross, precision=PRECISE),
            dot_t(w_own, cross, precision=PRECISE) + dot(w_far, far_cols, precision=PRECISE),
        ],
        axis=1,
    )
    margin = jnp.sqrt(jnp.sum(weighted * image, axis=1, keepdims=True) + 1e-06)
    first = lax.axis_index("trades") * NSET_DEV - 1
    costs = fund[...]
    lanes = lax.broadcasted_iota(jnp.int32, costs.shape, 1)
    cost = jnp.concatenate(
        [
            jnp.sum(jnp.where(lanes == first + w, costs, 0.0), axis=1, keepdims=True)
            for w in range(SPAN)
        ],
        axis=0,
    )
    weighted_bar = (cost / margin) * image
    conc_bar = dot_t(weighted_bar * risk * netted, hot, precision=PRECISE)
    sign = jnp.where(bucket_sum > 0.0, 1.0, jnp.where(bucket_sum < 0.0, -1.0, 0.0))
    bucket_bar = jnp.where(raw_ratio > 1.0, conc_bar * sign / (2.0 * limit * concentration), 0.0)
    bar_out[...] = (weighted_bar * scaled + dot(bucket_bar, hot, precision=PRECISE)).astype(BF16)
    grad = weighted_bar[scen:, :half] * netted[scen:, :half] * conc_factor[scen:, :half]
    weight_out[...] = jnp.broadcast_to(jnp.sum(grad, axis=0, keepdims=True), weight_out.shape)


def pull_kernel(bar, mine, other, where, money, side, state_out):
    scen, trades = money.shape
    double = 2 * trades
    half = side.shape[1]
    place = where[:1]
    spread = dot_t(bar[:, :half], mine[:double]) + dot_t(bar[:, half:], other[:double])
    pulled = jnp.zeros((scen, double), F32)
    for w in range(SPAN):
        pulled = pulled + jnp.where(place == w, spread[w * scen : (w + 1) * scen], 0.0)
    likely = lax.logistic(money[...])
    money_bar = (pulled[:, :trades] * likely * (1.0 - likely) + pulled[:, trades:]).astype(BF16)
    state_out[...] = dot(money_bar, side[...]).astype(BF16)


def near_vmem(x):
    return pltpu.with_memory_space_constraint(x, pltpu.VMEM)


def call(body, out_shape, *args, smem=()):
    return pl.pallas_call(
        body,
        out_shape=out_shape,
        in_specs=[
            pl.BlockSpec(memory_space=pltpu.SMEM if i in smem else pltpu.VMEM)
            for i in range(len(args))
        ],
        out_specs=jax.tree.map(lambda _: pl.BlockSpec(memory_space=pltpu.VMEM), out_shape),
    )(*args)


def shifted(x, axis, by):
    size = lax.axis_size(axis)
    pairs = [(i, i + by) for i in range(size) if 0 <= i + by < size]
    return lax.ppermute(x, axis, pairs)


def sum_over_trades(part):
    devs = lax.axis_size("trades")
    blocks = devs // NEAR
    place = lambda b, j: (b * NEAR + j - NEAR // 2) % devs
    mine = ((lax.axis_index("trades") + NEAR // 2) % devs) // NEAR
    groups = [[place(b, j) for j in range(NEAR)] for b in range(blocks)]
    copies = jnp.broadcast_to(part[None], (NEAR, *part.shape))
    got = lax.all_to_all(copies, "trades", 0, 0, tiled=True, axis_index_groups=groups)
    total = jnp.sum(got.astype(F32), axis=0)

    def send(x, *links):
        pairs = [(place(a, j), place(b, j)) for a, b in links for j in range(NEAR)]
        return lax.ppermute(x, "trades", pairs)

    def add(x, *links):
        return x + send(x.astype(BF16), *links).astype(F32)

    total = add(total, (4, 3), (2, 1))
    total = add(total, (5, 3), (6, 7))
    total = add(total, (3, 1))
    out = total.astype(BF16)
    whole = (total + send(out, (7, 0)).astype(F32) + send(out, (1, 0)).astype(F32)).astype(BF16)
    first = send(whole, (0, 1))
    second = send(whole, (0, 2))
    third = send(whole, (0, 3))
    first, second, third = lax.optimization_barrier((first, second, third))
    fourth = send(jnp.where(mine == 3, third, second), (3, 4), (2, 7))
    fifth = send(fourth, (4, 5), (7, 6))
    return jnp.where(mine == 0, whole, first + second + third + fourth + fifth)


def on_device(
    scenario_state,
    direction,
    trade_load,
    trade_curve,
    trade_set,
    factor_bucket_index,
    threshold,
    factor_risk_weight,
    correlation,
    funding,
):
    scen, set_count = funding.shape
    trades, half = trade_load.shape
    double, factors = 2 * trades, 2 * half
    mine = call(
        pack_kernel,
        pltpu.VMEM((double + 3 * half + 32, half), BF16),
        trade_load, trade_curve, correlation,
        factor_risk_weight.reshape(1, half), factor_bucket_index.reshape(1, half),
    )
    other = lax.ppermute(mine, "fact", [(0, 1), (1, 0)])
    money, pair, side, corr, where, fund, limit = call(
        money_kernel,
        (
            pltpu.VMEM((scen, trades), F32),
            pltpu.VMEM((scen, double), BF16),
            pltpu.VMEM((trades, half), BF16),
            pltpu.VMEM((factors, half), F32),
            pltpu.VMEM((8, double), jnp.int32),
            pltpu.VMEM(funding.shape, F32),
            pltpu.VMEM((8, 128), F32),
        ),
        near_vmem(scenario_state), near_vmem(direction), near_vmem(correlation),
        near_vmem(trade_set.reshape(1, trades)), near_vmem(funding), threshold,
        smem=(5,),
    )
    mine, other = near_vmem(mine), near_vmem(other)
    money, pair, side, corr, where, fund, limit = map(
        near_vmem, (money, pair, side, corr, where, fund, limit)
    )
    low, mid, high = call(
        window_kernel,
        (
            pltpu.VMEM((scen, factors), F32),
            pltpu.VMEM(((SPAN - 2) * scen, factors), F32),
            pltpu.VMEM((scen, factors), F32),
        ),
        pair, where, mine, other,
    )
    below = near_vmem(shifted(low, "trades", -1))
    above = near_vmem(shifted(high, "trades", 1))
    low, mid, high = near_vmem(low), near_vmem(mid), near_vmem(high)
    bar, weight = call(
        sets_kernel,
        (pltpu.VMEM((SPAN * scen, factors), BF16), pltpu.VMEM((8, half), F32)),
        low, mid, high, above, below, mine, other, corr, fund, limit,
    )
    for step in (1, 2):
        pairs = [(i, i ^ step) for i in range(lax.axis_size("scen"))]
        weight = weight + lax.ppermute(weight, "scen", pairs)
    state_part = call(
        pull_kernel,
        pltpu.VMEM((scen, half), BF16),
        near_vmem(bar), mine, other, where, money, side,
    )
    total = sum_over_trades(jnp.concatenate([state_part, weight.astype(BF16)], axis=0)).astype(F32)
    weight_grad = total[scen] / (scen * lax.axis_size("scen") * set_count)
    return (total[:scen], weight_grad)


def solution(mesh):
    placed = (
        P(("groups", "scen"), None),
        P("trades", None),
        P("trades", "fact"),
        P("trades", "fact"),
        P("trades"),
        P("fact"),
        P(),
        P("fact"),
        P(None, "fact"),
        P(("groups", "scen"), None),
    )
    return jax.shard_map(
        on_device,
        mesh=mesh,
        in_specs=placed,
        out_specs=(P(("groups", "scen"), "fact"), P(("groups", "fact"))),
        check_vma=False,
    )
```

```python
import jax
import jax.numpy as jnp
from jax import lax
from jax.experimental import pallas as pl
from jax.experimental.pallas import tpu as pltpu
from jax.sharding import PartitionSpec as P

NSET_DEV = 4
SPAN = NSET_DEV + 1
NEAR = 4
F32 = jnp.float32
BF16 = jnp.bfloat16
PRECISE = lax.Precision.HIGHEST


def three_parts(x):
    high = x.astype(BF16)
    rest = x - high.astype(F32)
    mid = rest.astype(BF16)
    low = (rest - mid.astype(F32)).astype(BF16)
    return high, mid, low


def from_parts(high, mid, low):
    return high.astype(F32) + mid.astype(F32) + low.astype(F32)


def dot_t(a, b, **kw):
    return lax.dot_general(a, b, (((1,), (1,)), ((), ())), preferred_element_type=F32, **kw)


def dot(a, b, **kw):
    return lax.dot_general(a, b, (((1,), (0,)), ((), ())), preferred_element_type=F32, **kw)


def pack_kernel(load, curve, corr, risk, bucket, out):
    trades, half = load.shape
    start = pl.multiple_of(lax.axis_index("fact") * half, half)
    out[:trades] = load[...]
    out[trades : 2 * trades] = curve[...]
    for i, part in enumerate(three_parts(corr[pl.ds(start, half)])):
        out[2 * trades + i * half : 2 * trades + (i + 1) * half] = part
    base = 2 * trades + 3 * half
    high, mid, low = three_parts(risk[...])
    for i, row in enumerate((high, mid, low, bucket[...].astype(F32).astype(BF16))):
        out[base + 8 * i : base + 8 * (i + 1)] = jnp.broadcast_to(row, (8, half))


def money_kernel(
    state, direction, corr, sets, funding, threshold,
    money_out, pair_out, side_out, corr_out, where_out, fund_out, limit_out,
):
    money = dot_t(state[...], direction[...])
    money_out[...] = money
    trades, factors = direction.shape
    half = factors // 2
    pair_out[:, :trades] = lax.logistic(money).astype(BF16)
    pair_out[:, trades:] = money.astype(BF16)
    side = pl.multiple_of(lax.axis_index("fact") * half, half)
    side_out[...] = direction[:, pl.ds(side, half)]
    corr_out[...] = corr[...]
    first = lax.axis_index("trades") * NSET_DEV - 1
    place = jnp.broadcast_to(sets[...] - first, (8, trades))
    where_out[:, :trades] = place
    where_out[:, trades:] = place
    fund_out[...] = funding[...]
    buckets = lax.broadcasted_iota(jnp.int32, limit_out.shape, 1)
    limit = jnp.ones(limit_out.shape, F32)
    for i in range(threshold.shape[0]):
        limit = jnp.where(buckets == i, threshold[i], limit)
    limit_out[...] = limit


def window_kernel(pair, where, mine, other, low_out, mid_out, high_out):
    scen, double = pair.shape
    paired = pair[...]
    place = where[:1]
    half = mine.shape[1]
    for w in range(SPAN):
        member = jnp.where(place == w, 1.0, 0.0).astype(BF16)
        mixing = paired * member
        if w == 0:
            out, at = low_out, 0
        elif w < SPAN - 1:
            out, at = mid_out, (w - 1) * scen
        else:
            out, at = high_out, 0
        out[at : at + scen, :half] = dot(mixing, mine[:double])
        out[at : at + scen, half:] = dot(mixing, other[:double])


def sets_kernel(
    low, mid, high, above, below, mine, other, corr, fund, limits, where, money, side_of, out
):
    scen, factors = low.shape
    half = factors // 2
    double = mine.shape[0] - 3 * half - 32
    side = pl.multiple_of(lax.axis_index("fact") * half, half)
    far_side = pl.multiple_of((1 - lax.axis_index("fact")) * half, half)
    netted = jnp.concatenate([low[...] + above[...], mid[...], high[...] + below[...]], axis=0)
    base = double + 3 * half

    def risk_of(ref):
        return from_parts(ref[base : base + 1], ref[base + 8 : base + 9], ref[base + 16 : base + 17])

    def bucket_of(ref):
        return ref[base + 24 : base + 25].astype(F32)

    risk = jnp.concatenate([risk_of(mine), risk_of(other)], axis=1)
    bucket = jnp.concatenate([bucket_of(mine), bucket_of(other)], axis=1).astype(jnp.int32)
    hot = jnp.where(
        lax.broadcasted_iota(jnp.int32, (16, factors), 0) == bucket, 1.0, 0.0
    ).astype(F32)
    limit = limits[:1, :16]
    bucket_sum = dot_t(netted, hot, precision=PRECISE)
    raw_ratio = jnp.sqrt(jnp.abs(bucket_sum) / limit)
    concentration = jnp.maximum(1.0, raw_ratio)
    conc_factor = dot(concentration, hot, precision=PRECISE)
    scaled = risk * conc_factor
    weighted = scaled * netted
    near_cols = corr[pl.ds(side, half)]
    cross = corr[pl.ds(far_side, half)]
    far_cols = from_parts(*[other[double + i * half : double + (i + 1) * half] for i in range(3)])
    w_own, w_far = weighted[:, :half], weighted[:, half:]
    image = jnp.concatenate(
        [
            dot(w_own, near_cols, precision=PRECISE) + dot(w_far, cross, precision=PRECISE),
            dot_t(w_own, cross, precision=PRECISE) + dot(w_far, far_cols, precision=PRECISE),
        ],
        axis=1,
    )
    margin = jnp.sqrt(jnp.sum(weighted * image, axis=1, keepdims=True) + 1e-06)
    first = lax.axis_index("trades") * NSET_DEV - 1
    costs = fund[...]
    lanes = lax.broadcasted_iota(jnp.int32, costs.shape, 1)
    cost = jnp.concatenate(
        [
            jnp.sum(jnp.where(lanes == first + w, costs, 0.0), axis=1, keepdims=True)
            for w in range(SPAN)
        ],
        axis=0,
    )
    weighted_bar = (cost / margin) * image
    conc_bar = dot_t(weighted_bar * risk * netted, hot, precision=PRECISE)
    sign = jnp.where(bucket_sum > 0.0, 1.0, jnp.where(bucket_sum < 0.0, -1.0, 0.0))
    bucket_bar = jnp.where(raw_ratio > 1.0, conc_bar * sign / (2.0 * limit * concentration), 0.0)
    bar = (weighted_bar * scaled + dot(bucket_bar, hot, precision=PRECISE)).astype(BF16)
    grad = weighted_bar[scen:, :half] * netted[scen:, :half] * conc_factor[scen:, :half]
    weight = jnp.broadcast_to(jnp.sum(grad, axis=0, keepdims=True), (8, half)).astype(BF16)
    trades = side_of.shape[0]
    place = where[:1]
    spread = dot_t(bar[:, :half], mine[:double]) + dot_t(bar[:, half:], other[:double])
    pulled = jnp.zeros((scen, double), F32)
    for w in range(SPAN):
        pulled = pulled + jnp.where(place == w, spread[w * scen : (w + 1) * scen], 0.0)
    likely = lax.logistic(money[...])
    money_bar = (pulled[:, :trades] * likely * (1.0 - likely) + pulled[:, trades:]).astype(BF16)
    state = dot(money_bar, side_of[...]).astype(BF16)
    for i in range(out.shape[0]):
        out[i, :scen] = state
        out[i, scen:] = weight


def near_vmem(x):
    return pltpu.with_memory_space_constraint(x, pltpu.VMEM)


def call(body, out_shape, *args, smem=()):
    return pl.pallas_call(
        body,
        out_shape=out_shape,
        in_specs=[
            pl.BlockSpec(memory_space=pltpu.SMEM if i in smem else pltpu.VMEM)
            for i in range(len(args))
        ],
        out_specs=jax.tree.map(lambda _: pl.BlockSpec(memory_space=pltpu.VMEM), out_shape),
    )(*args)


def shifted(x, axis, by):
    size = lax.axis_size(axis)
    pairs = [(i, i + by) for i in range(size) if 0 <= i + by < size]
    return lax.ppermute(x, axis, pairs)


def sum_over_trades(copies):
    devs = lax.axis_size("trades")
    blocks = devs // NEAR
    place = lambda b, j: (b * NEAR + j - NEAR // 2) % devs
    mine = ((lax.axis_index("trades") + NEAR // 2) % devs) // NEAR
    groups = [[place(b, j) for j in range(NEAR)] for b in range(blocks)]
    got = lax.all_to_all(copies, "trades", 0, 0, tiled=True, axis_index_groups=groups)
    total = jnp.sum(got.astype(F32), axis=0)

    def send(x, *links):
        pairs = [(place(a, j), place(b, j)) for a, b in links for j in range(NEAR)]
        return lax.ppermute(x, "trades", pairs)

    def add(x, *links):
        return x + send(x.astype(BF16), *links).astype(F32)

    total = add(total, (4, 3), (2, 1))
    total = add(total, (5, 3), (6, 7))
    total = add(total, (3, 1))
    out = total.astype(BF16)
    whole = (total + send(out, (7, 0)).astype(F32) + send(out, (1, 0)).astype(F32)).astype(BF16)
    def spread(x, target):
        pairs = [(place(0, NEAR - 1 - j), place(target, j)) for j in range(NEAR)]
        return lax.ppermute(x, "trades", pairs)

    first = spread(whole, 1)
    second = spread(whole, 2)
    third = spread(whole, 3)
    first, second, third = lax.optimization_barrier((first, second, third))
    fourth = send(jnp.where(mine == 3, third, second), (3, 4), (2, 7))
    fifth = send(fourth, (4, 5), (7, 6))
    return jnp.where(mine == 0, whole, first + second + third + fourth + fifth)


def on_device(
    scenario_state,
    direction,
    trade_load,
    trade_curve,
    trade_set,
    factor_bucket_index,
    threshold,
    factor_risk_weight,
    correlation,
    funding,
):
    scen, set_count = funding.shape
    trades, half = trade_load.shape
    double, factors = 2 * trades, 2 * half
    mine = call(
        pack_kernel,
        pltpu.VMEM((double + 3 * half + 32, half), BF16),
        trade_load, trade_curve, correlation,
        factor_risk_weight.reshape(1, half), factor_bucket_index.reshape(1, half),
    )
    other = lax.ppermute(mine, "fact", [(0, 1), (1, 0)])
    money, pair, side, corr, where, fund, limit = call(
        money_kernel,
        (
            pltpu.VMEM((scen, trades), F32),
            pltpu.VMEM((scen, double), BF16),
            pltpu.VMEM((trades, half), BF16),
            pltpu.VMEM((factors, half), F32),
            pltpu.VMEM((8, double), jnp.int32),
            pltpu.VMEM(funding.shape, F32),
            pltpu.VMEM((8, 128), F32),
        ),
        near_vmem(scenario_state), near_vmem(direction), near_vmem(correlation),
        near_vmem(trade_set.reshape(1, trades)), near_vmem(funding), threshold,
        smem=(5,),
    )
    mine, other = near_vmem(mine), near_vmem(other)
    money, pair, side, corr, where, fund, limit = map(
        near_vmem, (money, pair, side, corr, where, fund, limit)
    )
    low, mid, high = call(
        window_kernel,
        (
            pltpu.VMEM((scen, factors), F32),
            pltpu.VMEM(((SPAN - 2) * scen, factors), F32),
            pltpu.VMEM((scen, factors), F32),
        ),
        pair, where, mine, other,
    )
    below, above = lax.optimization_barrier(
        (shifted(low, "trades", -1), shifted(high, "trades", 1))
    )
    below, above = near_vmem(below), near_vmem(above)
    low, mid, high = near_vmem(low), near_vmem(mid), near_vmem(high)
    copies = call(
        sets_kernel,
        pltpu.VMEM((NEAR, scen + 8, half), BF16),
        low, mid, high, above, below, mine, other, corr, fund, limit, where, money, side,
    )
    total = sum_over_trades(copies)
    cols = lax.axis_size("scen")
    copies = jnp.broadcast_to(total[scen:][None], (cols, 8, half))
    weight_sum = jnp.sum(lax.all_to_all(copies, "scen", 0, 0, tiled=True).astype(F32), axis=0)[0]
    total, weight_sum = lax.optimization_barrier((total, weight_sum))
    weight_grad = weight_sum / (scen * cols * set_count)
    return (total[:scen].astype(F32), weight_grad)


def solution(mesh):
    placed = (
        P(("groups", "scen"), None),
        P("trades", None),
        P("trades", "fact"),
        P("trades", "fact"),
        P("trades"),
        P("fact"),
        P(),
        P("fact"),
        P(None, "fact"),
        P(("groups", "scen"), None),
    )
    return jax.shard_map(
        on_device,
        mesh=mesh,
        in_specs=placed,
        out_specs=(P(("groups", "scen"), "fact"), P(("groups", "fact"))),
        check_vma=False,
    )
```

```python
import functools

import jax
import jax.numpy as jnp
from jax import lax
from jax.experimental import pallas as pl
from jax.experimental.pallas import tpu as pltpu
from jax.sharding import PartitionSpec as P

NSET_DEV = 4
SPAN = NSET_DEV + 1
NEAR = 4
F32 = jnp.float32
BF16 = jnp.bfloat16
PRECISE = lax.Precision.HIGHEST


def three_parts(x):
    high = x.astype(BF16)
    rest = x - high.astype(F32)
    mid = rest.astype(BF16)
    low = (rest - mid.astype(F32)).astype(BF16)
    return high, mid, low


def from_parts(high, mid, low):
    return high.astype(F32) + mid.astype(F32) + low.astype(F32)


def dot_t(a, b, **kw):
    return lax.dot_general(a, b, (((1,), (1,)), ((), ())), preferred_element_type=F32, **kw)


def dot(a, b, **kw):
    return lax.dot_general(a, b, (((1,), (0,)), ((), ())), preferred_element_type=F32, **kw)


def pack_kernel(load, curve, corr, risk, bucket, out):
    trades, half = load.shape
    start = pl.multiple_of(lax.axis_index("fact") * half, half)
    out[:trades] = load[...]
    out[trades : 2 * trades] = curve[...]
    for i, part in enumerate(three_parts(corr[pl.ds(start, half)])):
        out[2 * trades + i * half : 2 * trades + (i + 1) * half] = part
    base = 2 * trades + 3 * half
    high, mid, low = three_parts(risk[...])
    for i, row in enumerate((high, mid, low, bucket[...].astype(F32).astype(BF16))):
        out[base + 8 * i : base + 8 * (i + 1)] = jnp.broadcast_to(row, (8, half))


def money_kernel(
    state, direction, corr, sets, funding, threshold,
    money_out, pair_out, side_out, corr_out, where_out, fund_out, limit_out,
):
    money = dot_t(state[...], direction[...])
    money_out[...] = money
    trades, factors = direction.shape
    half = factors // 2
    pair_out[:, :trades] = lax.logistic(money).astype(BF16)
    pair_out[:, trades:] = money.astype(BF16)
    side = pl.multiple_of(lax.axis_index("fact") * half, half)
    side_out[...] = direction[:, pl.ds(side, half)]
    corr_out[...] = corr[...]
    first = lax.axis_index("trades") * NSET_DEV - 1
    place = jnp.broadcast_to(sets[...] - first, (8, trades))
    where_out[:, :trades] = place
    where_out[:, trades:] = place
    fund_out[...] = funding[...]
    buckets = lax.broadcasted_iota(jnp.int32, limit_out.shape, 1)
    limit = jnp.ones(limit_out.shape, F32)
    for i in range(threshold.shape[0]):
        limit = jnp.where(buckets == i, threshold[i], limit)
    limit_out[...] = limit


def window_kernel(pair, where, mine, other, low_out, mid_out, high_out):
    scen, double = pair.shape
    paired = pair[...]
    place = where[:1]
    half = mine.shape[1]
    for w in range(SPAN):
        member = jnp.where(place == w, 1.0, 0.0).astype(BF16)
        mixing = paired * member
        if w == 0:
            out, at = low_out, 0
        elif w < SPAN - 1:
            out, at = mid_out, (w - 1) * scen
        else:
            out, at = high_out, 0
        out[at : at + scen, :half] = dot(mixing, mine[:double])
        out[at : at + scen, half:] = dot(mixing, other[:double])


def sets_kernel(
    low, mid, high, above, below, mine, other, corr, fund, limits, where, money, side_of, out
):
    scen, factors = low.shape
    half = factors // 2
    double = mine.shape[0] - 3 * half - 32
    side = pl.multiple_of(lax.axis_index("fact") * half, half)
    far_side = pl.multiple_of((1 - lax.axis_index("fact")) * half, half)
    netted = jnp.concatenate([low[...] + above[...], mid[...], high[...] + below[...]], axis=0)
    base = double + 3 * half

    def risk_of(ref):
        return from_parts(ref[base : base + 1], ref[base + 8 : base + 9], ref[base + 16 : base + 17])

    def bucket_of(ref):
        return ref[base + 24 : base + 25].astype(F32)

    risk = jnp.concatenate([risk_of(mine), risk_of(other)], axis=1)
    bucket = jnp.concatenate([bucket_of(mine), bucket_of(other)], axis=1).astype(jnp.int32)
    hot = jnp.where(
        lax.broadcasted_iota(jnp.int32, (16, factors), 0) == bucket, 1.0, 0.0
    ).astype(F32)
    limit = limits[:1, :16]
    bucket_sum = dot_t(netted, hot, precision=PRECISE)
    raw_ratio = jnp.sqrt(jnp.abs(bucket_sum) / limit)
    concentration = jnp.maximum(1.0, raw_ratio)
    conc_factor = dot(concentration, hot, precision=PRECISE)
    scaled = risk * conc_factor
    weighted = scaled * netted
    near_cols = corr[pl.ds(side, half)]
    cross = corr[pl.ds(far_side, half)]
    far_cols = from_parts(*[other[double + i * half : double + (i + 1) * half] for i in range(3)])
    w_own, w_far = weighted[:, :half], weighted[:, half:]
    image = jnp.concatenate(
        [
            dot(w_own, near_cols, precision=PRECISE) + dot(w_far, cross, precision=PRECISE),
            dot_t(w_own, cross, precision=PRECISE) + dot(w_far, far_cols, precision=PRECISE),
        ],
        axis=1,
    )
    margin = jnp.sqrt(jnp.sum(weighted * image, axis=1, keepdims=True) + 1e-06)
    first = lax.axis_index("trades") * NSET_DEV - 1
    costs = fund[...]
    lanes = lax.broadcasted_iota(jnp.int32, costs.shape, 1)
    cost = jnp.concatenate(
        [
            jnp.sum(jnp.where(lanes == first + w, costs, 0.0), axis=1, keepdims=True)
            for w in range(SPAN)
        ],
        axis=0,
    )
    weighted_bar = (cost / margin) * image
    conc_bar = dot_t(weighted_bar * risk * netted, hot, precision=PRECISE)
    sign = jnp.where(bucket_sum > 0.0, 1.0, jnp.where(bucket_sum < 0.0, -1.0, 0.0))
    bucket_bar = jnp.where(raw_ratio > 1.0, conc_bar * sign / (2.0 * limit * concentration), 0.0)
    bar = (weighted_bar * scaled + dot(bucket_bar, hot, precision=PRECISE)).astype(BF16)
    grad = weighted_bar[scen:, :half] * netted[scen:, :half] * conc_factor[scen:, :half]
    weight = jnp.broadcast_to(jnp.sum(grad, axis=0, keepdims=True), (8, half)).astype(BF16)
    trades = side_of.shape[0]
    place = where[:1]
    spread = dot_t(bar[:, :half], mine[:double]) + dot_t(bar[:, half:], other[:double])
    pulled = jnp.zeros((scen, double), F32)
    for w in range(SPAN):
        pulled = pulled + jnp.where(place == w, spread[w * scen : (w + 1) * scen], 0.0)
    likely = lax.logistic(money[...])
    money_bar = (pulled[:, :trades] * likely * (1.0 - likely) + pulled[:, trades:]).astype(BF16)
    state = dot(money_bar, side_of[...]).astype(BF16)
    for i in range(out.shape[0]):
        out[i, :scen] = state
        out[i, scen:] = weight


def fold_kernel(got, total_out):
    count, rows, half = got.shape
    cols = count // NEAR
    scen = rows - 8
    mine = lax.axis_index("scen")
    state = jnp.zeros((scen, half), F32)
    for j in range(NEAR):
        state = state + got[j * cols + mine, :scen].astype(F32)
    weight = jnp.zeros((8, half), F32)
    for i in range(count):
        weight = weight + got[i, scen:].astype(F32)
    total_out[:scen] = state
    total_out[scen:] = weight


def last_kernel(count, whole, first, second, third, fourth, state_out, weight_out):
    scen = state_out.shape[0]
    devs = lax.axis_size("trades")
    late = lax.rem(lax.axis_index("trades") + NEAR // 2, devs) < NEAR
    parts = [x[...].astype(F32) for x in (whole, first, second, third, fourth)]
    total = jnp.where(late, parts[0], parts[1] + parts[2] + parts[3] + parts[4])
    state_out[...] = total[:scen]
    weight_out[...] = total[scen : scen + 1] * (1.0 / count)


def near_vmem(x):
    return pltpu.with_memory_space_constraint(x, pltpu.VMEM)


def call(body, out_shape, *args, smem=()):
    return pl.pallas_call(
        body,
        out_shape=out_shape,
        in_specs=[
            pl.BlockSpec(memory_space=pltpu.SMEM if i in smem else pltpu.VMEM)
            for i in range(len(args))
        ],
        out_specs=jax.tree.map(lambda _: pl.BlockSpec(memory_space=pltpu.VMEM), out_shape),
    )(*args)


def shifted(x, axis, by):
    size = lax.axis_size(axis)
    pairs = [(i, i + by) for i in range(size) if 0 <= i + by < size]
    return lax.ppermute(x, axis, pairs)


def sum_over_trades(copies):
    devs, cols = lax.axis_size("trades"), lax.axis_size("scen")
    blocks = devs // NEAR
    place = lambda b, j: (b * NEAR + j - NEAR // 2) % devs
    mine = lax.rem(lax.axis_index("trades") + NEAR // 2, devs) // NEAR
    groups = [
        [place(b, j) * cols + c for j in range(NEAR) for c in range(cols)] for b in range(blocks)
    ]
    got = lax.all_to_all(copies, ("trades", "scen"), 0, 0, tiled=True, axis_index_groups=groups)
    total = call(fold_kernel, pltpu.VMEM(copies.shape[1:], F32), near_vmem(got))

    def send(x, *links):
        pairs = []
        for a, b, flip in links:
            pairs += [(place(a, NEAR - 1 - j if flip else j), place(b, j)) for j in range(NEAR)]
        return lax.ppermute(x.astype(BF16), "trades", pairs)

    total = total + send(total, (4, 3, 0), (2, 1, 0)).astype(F32)
    one, two = lax.optimization_barrier(
        (send(total, (5, 1, 0), (6, 7, 0)), send(total, (3, 1, 0)))
    )
    total = total + one.astype(F32) + two.astype(F32)
    one, two = lax.optimization_barrier((send(total, (7, 0, 0)), send(total, (1, 0, 0))))
    whole = (total + one.astype(F32) + two.astype(F32)).astype(BF16)
    first, second = lax.optimization_barrier((send(whole, (0, 1, 1)), send(whole, (0, 2, 1))))
    have = jnp.where(mine == 1, first, jnp.where(mine == 2, second, whole))
    third = send(have, (0, 4, 1), (1, 3, 0), (2, 7, 0))
    fourth = send(third, (4, 5, 0), (7, 6, 0))
    return whole, first, second, third, fourth


def on_device(
    scenario_state,
    direction,
    trade_load,
    trade_curve,
    trade_set,
    factor_bucket_index,
    threshold,
    factor_risk_weight,
    correlation,
    funding,
):
    scen, set_count = funding.shape
    trades, half = trade_load.shape
    double, factors = 2 * trades, 2 * half
    mine = call(
        pack_kernel,
        pltpu.VMEM((double + 3 * half + 32, half), BF16),
        trade_load, trade_curve, correlation,
        factor_risk_weight.reshape(1, half), factor_bucket_index.reshape(1, half),
    )
    other = lax.ppermute(mine, "fact", [(0, 1), (1, 0)])
    money, pair, side, corr, where, fund, limit = call(
        money_kernel,
        (
            pltpu.VMEM((scen, trades), F32),
            pltpu.VMEM((scen, double), BF16),
            pltpu.VMEM((trades, half), BF16),
            pltpu.VMEM((factors, half), F32),
            pltpu.VMEM((8, double), jnp.int32),
            pltpu.VMEM(funding.shape, F32),
            pltpu.VMEM((8, 128), F32),
        ),
        near_vmem(scenario_state), near_vmem(direction), near_vmem(correlation),
        near_vmem(trade_set.reshape(1, trades)), near_vmem(funding), threshold,
        smem=(5,),
    )
    mine, other = near_vmem(mine), near_vmem(other)
    money, pair, side, corr, where, fund, limit = map(
        near_vmem, (money, pair, side, corr, where, fund, limit)
    )
    low, mid, high = call(
        window_kernel,
        (
            pltpu.VMEM((scen, factors), F32),
            pltpu.VMEM(((SPAN - 2) * scen, factors), F32),
            pltpu.VMEM((scen, factors), F32),
        ),
        pair, where, mine, other,
    )
    below, above = lax.optimization_barrier(
        (shifted(low, "trades", -1), shifted(high, "trades", 1))
    )
    below, above = near_vmem(below), near_vmem(above)
    low, mid, high = near_vmem(low), near_vmem(mid), near_vmem(high)
    copies = call(
        sets_kernel,
        pltpu.VMEM((NEAR * lax.axis_size("scen"), scen + 8, half), BF16),
        low, mid, high, above, below, mine, other, corr, fund, limit, where, money, side,
    )
    count = scen * lax.axis_size("scen") * set_count
    state_grad, weight_grad = call(
        functools.partial(last_kernel, count),
        (jax.ShapeDtypeStruct((scen, half), F32), jax.ShapeDtypeStruct((1, half), F32)),
        *map(near_vmem, sum_over_trades(copies)),
    )
    return (state_grad, weight_grad.reshape(half))


def solution(mesh):
    placed = (
        P(("groups", "scen"), None),
        P("trades", None),
        P("trades", "fact"),
        P("trades", "fact"),
        P("trades"),
        P("fact"),
        P(),
        P("fact"),
        P(None, "fact"),
        P(("groups", "scen"), None),
    )
    return jax.shard_map(
        on_device,
        mesh=mesh,
        in_specs=placed,
        out_specs=(P(("groups", "scen"), "fact"), P(("groups", "fact"))),
        check_vma=False,
    )
```

```python
import functools

import jax
import jax.numpy as jnp
from jax import lax
from jax.experimental import pallas as pl
from jax.experimental.pallas import tpu as pltpu
from jax.sharding import PartitionSpec as P

NSET_DEV = 4
SPAN = NSET_DEV + 1
NEAR = 4
F32 = jnp.float32
BF16 = jnp.bfloat16
PRECISE = lax.Precision.HIGHEST


def three_parts(x):
    high = x.astype(BF16)
    rest = x - high.astype(F32)
    mid = rest.astype(BF16)
    low = (rest - mid.astype(F32)).astype(BF16)
    return high, mid, low


def from_parts(high, mid, low):
    return high.astype(F32) + mid.astype(F32) + low.astype(F32)


def dot_t(a, b, **kw):
    return lax.dot_general(a, b, (((1,), (1,)), ((), ())), preferred_element_type=F32, **kw)


def dot(a, b, **kw):
    return lax.dot_general(a, b, (((1,), (0,)), ((), ())), preferred_element_type=F32, **kw)


def pack_kernel(load, curve, corr, risk, bucket, out):
    trades, half = load.shape
    start = pl.multiple_of(lax.axis_index("fact") * half, half)
    out[:trades] = load[...]
    out[trades : 2 * trades] = curve[...]
    for i, part in enumerate(three_parts(corr[pl.ds(start, half)])):
        out[2 * trades + i * half : 2 * trades + (i + 1) * half] = part
    base = 2 * trades + 3 * half
    high, mid, low = three_parts(risk[...])
    for i, row in enumerate((high, mid, low, bucket[...].astype(F32).astype(BF16))):
        out[base + 8 * i : base + 8 * (i + 1)] = jnp.broadcast_to(row, (8, half))


def money_kernel(
    state, direction, corr, sets, funding, threshold,
    money_out, pair_out, side_out, corr_out, where_out, fund_out, limit_out,
):
    money = dot_t(state[...], direction[...])
    money_out[...] = money
    trades, factors = direction.shape
    half = factors // 2
    pair_out[:, :trades] = lax.logistic(money).astype(BF16)
    pair_out[:, trades:] = money.astype(BF16)
    side = pl.multiple_of(lax.axis_index("fact") * half, half)
    side_out[...] = direction[:, pl.ds(side, half)]
    corr_out[...] = corr[...]
    first = lax.axis_index("trades") * NSET_DEV - 1
    place = jnp.broadcast_to(sets[...] - first, (8, trades))
    where_out[:, :trades] = place
    where_out[:, trades:] = place
    fund_out[...] = funding[...]
    buckets = lax.broadcasted_iota(jnp.int32, limit_out.shape, 1)
    limit = jnp.ones(limit_out.shape, F32)
    for i in range(threshold.shape[0]):
        limit = jnp.where(buckets == i, threshold[i], limit)
    limit_out[...] = limit


def window_kernel(pair, where, mine, other, low_out, mid_out, high_out, edge_out):
    scen, double = pair.shape
    paired = pair[...]
    place = where[:1]
    half = mine.shape[1]
    for w in range(SPAN):
        member = jnp.where(place == w, 1.0, 0.0).astype(BF16)
        mixing = paired * member
        if w == 0:
            out, at = low_out, 0
        elif w < SPAN - 1:
            out, at = mid_out, (w - 1) * scen
        else:
            out, at = high_out, 0
        out[at : at + scen, :half] = dot(mixing, mine[:double])
        out[at : at + scen, half:] = dot(mixing, other[:double])
    edge_out[...] = low_out[...]


def sets_kernel(
    low, mid, high, above, below, start, mine, other, corr, fund, limits, where, money, side_of, out
):
    scen, factors = low.shape
    half = factors // 2
    double = mine.shape[0] - 3 * half - 32
    side = pl.multiple_of(lax.axis_index("fact") * half, half)
    far_side = pl.multiple_of((1 - lax.axis_index("fact")) * half, half)
    netted = jnp.concatenate([low[...] + above[...], mid[...], high[...] + (below[...] + start[...])], axis=0)
    base = double + 3 * half

    def risk_of(ref):
        return from_parts(ref[base : base + 1], ref[base + 8 : base + 9], ref[base + 16 : base + 17])

    def bucket_of(ref):
        return ref[base + 24 : base + 25].astype(F32)

    risk = jnp.concatenate([risk_of(mine), risk_of(other)], axis=1)
    bucket = jnp.concatenate([bucket_of(mine), bucket_of(other)], axis=1).astype(jnp.int32)
    hot = jnp.where(
        lax.broadcasted_iota(jnp.int32, (16, factors), 0) == bucket, 1.0, 0.0
    ).astype(F32)
    limit = limits[:1, :16]
    bucket_sum = dot_t(netted, hot, precision=PRECISE)
    raw_ratio = jnp.sqrt(jnp.abs(bucket_sum) / limit)
    concentration = jnp.maximum(1.0, raw_ratio)
    conc_factor = dot(concentration, hot, precision=PRECISE)
    scaled = risk * conc_factor
    weighted = scaled * netted
    near_cols = corr[pl.ds(side, half)]
    cross = corr[pl.ds(far_side, half)]
    far_cols = from_parts(*[other[double + i * half : double + (i + 1) * half] for i in range(3)])
    w_own, w_far = weighted[:, :half], weighted[:, half:]
    image = jnp.concatenate(
        [
            dot(w_own, near_cols, precision=PRECISE) + dot(w_far, cross, precision=PRECISE),
            dot_t(w_own, cross, precision=PRECISE) + dot(w_far, far_cols, precision=PRECISE),
        ],
        axis=1,
    )
    margin = jnp.sqrt(jnp.sum(weighted * image, axis=1, keepdims=True) + 1e-06)
    first = lax.axis_index("trades") * NSET_DEV - 1
    costs = fund[...]
    lanes = lax.broadcasted_iota(jnp.int32, costs.shape, 1)
    cost = jnp.concatenate(
        [
            jnp.sum(jnp.where(lanes == first + w, costs, 0.0), axis=1, keepdims=True)
            for w in range(SPAN)
        ],
        axis=0,
    )
    weighted_bar = (cost / margin) * image
    conc_bar = dot_t(weighted_bar * risk * netted, hot, precision=PRECISE)
    sign = jnp.where(bucket_sum > 0.0, 1.0, jnp.where(bucket_sum < 0.0, -1.0, 0.0))
    bucket_bar = jnp.where(raw_ratio > 1.0, conc_bar * sign / (2.0 * limit * concentration), 0.0)
    bar = (weighted_bar * scaled + dot(bucket_bar, hot, precision=PRECISE)).astype(BF16)
    grad = weighted_bar[scen:, :half] * netted[scen:, :half] * conc_factor[scen:, :half]
    weight = jnp.broadcast_to(jnp.sum(grad, axis=0, keepdims=True), (8, half)).astype(BF16)
    trades = side_of.shape[0]
    place = where[:1]
    spread = dot_t(bar[:, :half], mine[:double]) + dot_t(bar[:, half:], other[:double])
    pulled = jnp.zeros((scen, double), F32)
    for w in range(SPAN):
        pulled = pulled + jnp.where(place == w, spread[w * scen : (w + 1) * scen], 0.0)
    likely = lax.logistic(money[...])
    money_bar = (pulled[:, :trades] * likely * (1.0 - likely) + pulled[:, trades:]).astype(BF16)
    state = dot(money_bar, side_of[...]).astype(BF16)
    for i in range(out.shape[0]):
        out[i, :scen] = state
        out[i, scen:] = weight


def fold_kernel(got, total_out):
    count, rows, half = got.shape
    cols = count // NEAR
    scen = rows - 8
    mine = lax.axis_index("scen")
    state = jnp.zeros((scen, half), F32)
    for j in range(NEAR):
        state = state + got[j * cols + mine, :scen].astype(F32)
    weight = jnp.zeros((8, half), F32)
    for i in range(count):
        weight = weight + got[i, scen:].astype(F32)
    total_out[:scen] = state
    total_out[scen:] = weight


def last_kernel(count, whole, first, second, third, fourth, state_out, weight_out):
    scen = state_out.shape[0]
    devs = lax.axis_size("trades")
    late = lax.rem(lax.axis_index("trades") + NEAR // 2, devs) < NEAR
    parts = [x[...].astype(F32) for x in (whole, first, second, third, fourth)]
    total = jnp.where(late, parts[0], parts[1] + parts[2] + parts[3] + parts[4])
    state_out[...] = total[:scen]
    weight_out[...] = total[scen : scen + 1] * (1.0 / count)


def near_vmem(x):
    return pltpu.with_memory_space_constraint(x, pltpu.VMEM)


def call(body, out_shape, *args, smem=()):
    return pl.pallas_call(
        body,
        out_shape=out_shape,
        in_specs=[
            pl.BlockSpec(memory_space=pltpu.SMEM if i in smem else pltpu.VMEM)
            for i in range(len(args))
        ],
        out_specs=jax.tree.map(lambda _: pl.BlockSpec(memory_space=pltpu.VMEM), out_shape),
    )(*args)


def shifted(x, axis, by, first=0):
    size = lax.axis_size(axis)
    pairs = [(i, i + by) for i in range(first, size) if 0 <= i + by < size]
    return lax.ppermute(x, axis, pairs)


def sum_over_trades(copies):
    devs, cols = lax.axis_size("trades"), lax.axis_size("scen")
    blocks = devs // NEAR
    place = lambda b, j: (b * NEAR + j - NEAR // 2) % devs
    mine = lax.rem(lax.axis_index("trades") + NEAR // 2, devs) // NEAR
    groups = [
        [place(b, j) * cols + c for j in range(NEAR) for c in range(cols)] for b in range(blocks)
    ]
    got = lax.all_to_all(copies, ("trades", "scen"), 0, 0, tiled=True, axis_index_groups=groups)
    total = call(fold_kernel, pltpu.VMEM(copies.shape[1:], F32), near_vmem(got))

    def send(x, *links):
        pairs = []
        for a, b, flip in links:
            pairs += [(place(a, NEAR - 1 - j if flip else j), place(b, j)) for j in range(NEAR)]
        return lax.ppermute(x.astype(BF16), "trades", pairs)

    far = send(total, (5, 1, 0))
    total = total + send(total, (6, 7, 0), (4, 3, 0), (2, 1, 0)).astype(F32)
    total = total + far.astype(F32) + send(total, (3, 1, 0)).astype(F32)
    one, two = lax.optimization_barrier((send(total, (7, 0, 0)), send(total, (1, 0, 0))))
    whole = (total + one.astype(F32) + two.astype(F32)).astype(BF16)
    second, first = lax.optimization_barrier((send(whole, (0, 2, 1)), send(whole, (0, 1, 1))))
    third = send(jnp.where(mine == 1, first, second), (1, 3, 0), (2, 5, 0))
    fourth = send(jnp.where(mine == 2, second, third), (3, 4, 0), (5, 6, 0), (2, 7, 0))
    return whole, first, second, third, fourth


def on_device(
    scenario_state,
    direction,
    trade_load,
    trade_curve,
    trade_set,
    factor_bucket_index,
    threshold,
    factor_risk_weight,
    correlation,
    funding,
):
    scen, set_count = funding.shape
    trades, half = trade_load.shape
    double, factors = 2 * trades, 2 * half
    mine = call(
        pack_kernel,
        pltpu.VMEM((double + 3 * half + 32, half), BF16),
        trade_load, trade_curve, correlation,
        factor_risk_weight.reshape(1, half), factor_bucket_index.reshape(1, half),
    )
    other = lax.ppermute(mine, "fact", [(0, 1), (1, 0)])
    money, pair, side, corr, where, fund, limit = call(
        money_kernel,
        (
            pltpu.VMEM((scen, trades), F32),
            pltpu.VMEM((scen, double), BF16),
            pltpu.VMEM((trades, half), BF16),
            pltpu.VMEM((factors, half), F32),
            pltpu.VMEM((8, double), jnp.int32),
            pltpu.VMEM(funding.shape, F32),
            pltpu.VMEM((8, 128), F32),
        ),
        near_vmem(scenario_state), near_vmem(direction), near_vmem(correlation),
        near_vmem(trade_set.reshape(1, trades)), near_vmem(funding), threshold,
        smem=(5,),
    )
    mine, other = near_vmem(mine), near_vmem(other)
    money, pair, side, corr, where, fund, limit = map(
        near_vmem, (money, pair, side, corr, where, fund, limit)
    )
    low, mid, high, edge = call(
        window_kernel,
        (
            pltpu.VMEM((scen, factors), F32),
            pltpu.VMEM(((SPAN - 2) * scen, factors), F32),
            pltpu.VMEM((scen, factors), F32),
            pltpu.VMEM((scen, factors), F32),
        ),
        pair, where, mine, other,
    )
    below, above, start = lax.optimization_barrier(
        (shifted(low, "trades", -1, 2), shifted(high, "trades", 1), lax.ppermute(edge, "trades", [(1, 0)]))
    )
    below, above, start = near_vmem(below), near_vmem(above), near_vmem(start)
    low, mid, high = near_vmem(low), near_vmem(mid), near_vmem(high)
    copies = call(
        sets_kernel,
        pltpu.VMEM((NEAR * lax.axis_size("scen"), scen + 8, half), BF16),
        low, mid, high, above, below, start, mine, other, corr, fund, limit, where, money, side,
    )
    count = scen * lax.axis_size("scen") * set_count
    state_grad, weight_grad = call(
        functools.partial(last_kernel, count),
        (jax.ShapeDtypeStruct((scen, half), F32), jax.ShapeDtypeStruct((1, half), F32)),
        *map(near_vmem, sum_over_trades(copies)),
    )
    return (state_grad, weight_grad.reshape(half))


def solution(mesh):
    placed = (
        P(("groups", "scen"), None),
        P("trades", None),
        P("trades", "fact"),
        P("trades", "fact"),
        P("trades"),
        P("fact"),
        P(),
        P("fact"),
        P(None, "fact"),
        P(("groups", "scen"), None),
    )
    return jax.shard_map(
        on_device,
        mesh=mesh,
        in_specs=placed,
        out_specs=(P(("groups", "scen"), "fact"), P(("groups", "fact"))),
        check_vma=False,
    )
```

```python
import functools

import jax
import jax.numpy as jnp
from jax import lax
from jax.experimental import pallas as pl
from jax.experimental.pallas import tpu as pltpu
from jax.sharding import PartitionSpec as P

NSET_DEV = 4
SPAN = NSET_DEV + 1
NEAR = 4
F32 = jnp.float32
BF16 = jnp.bfloat16
PRECISE = lax.Precision.HIGHEST


def three_parts(x):
    high = x.astype(BF16)
    rest = x - high.astype(F32)
    mid = rest.astype(BF16)
    low = (rest - mid.astype(F32)).astype(BF16)
    return high, mid, low


def from_parts(high, mid, low):
    return high.astype(F32) + mid.astype(F32) + low.astype(F32)


def dot_t(a, b, **kw):
    return lax.dot_general(a, b, (((1,), (1,)), ((), ())), preferred_element_type=F32, **kw)


def dot(a, b, **kw):
    return lax.dot_general(a, b, (((1,), (0,)), ((), ())), preferred_element_type=F32, **kw)


def pack_kernel(load, curve, corr, risk, bucket, out):
    trades, half = load.shape
    start = pl.multiple_of(lax.axis_index("fact") * half, half)
    out[:trades] = load[...]
    out[trades : 2 * trades] = curve[...]
    for i, part in enumerate(three_parts(corr[pl.ds(start, half)])):
        out[2 * trades + i * half : 2 * trades + (i + 1) * half] = part
    base = 2 * trades + 3 * half
    high, mid, low = three_parts(risk[...])
    for i, row in enumerate((high, mid, low, bucket[...].astype(F32).astype(BF16))):
        out[base + 8 * i : base + 8 * (i + 1)] = jnp.broadcast_to(row, (8, half))


def money_kernel(
    state, direction, corr, sets, funding, threshold,
    money_out, pair_out, side_out, corr_out, where_out, fund_out, limit_out,
):
    money = dot_t(state[...], direction[...])
    money_out[...] = money
    trades, factors = direction.shape
    half = factors // 2
    pair_out[:, :trades] = lax.logistic(money).astype(BF16)
    pair_out[:, trades:] = money.astype(BF16)
    side = pl.multiple_of(lax.axis_index("fact") * half, half)
    side_out[...] = direction[:, pl.ds(side, half)]
    far_side = pl.multiple_of((1 - lax.axis_index("fact")) * half, half)
    cross = corr[pl.ds(far_side, half)]
    corr_out[:half, :half] = corr[pl.ds(side, half)]
    corr_out[half:, :half] = cross
    corr_out[:half, half:] = cross.T
    first = lax.axis_index("trades") * NSET_DEV - 1
    place = jnp.broadcast_to(sets[...] - first, (8, trades))
    where_out[:, :trades] = place
    where_out[:, trades:] = place
    fund_out[...] = funding[...]
    buckets = lax.broadcasted_iota(jnp.int32, limit_out.shape, 1)
    limit = jnp.ones(limit_out.shape, F32)
    for i in range(threshold.shape[0]):
        limit = jnp.where(buckets == i, threshold[i], limit)
    limit_out[...] = limit


def window_kernel(pair, where, mine, other, net_out, low_out, high_out, edge_out):
    scen, double = pair.shape
    paired = pair[...]
    place = where[:1]
    half = mine.shape[1]
    for w in range(SPAN):
        member = jnp.where(place == w, 1.0, 0.0).astype(BF16)
        mixing = paired * member
        own = dot(mixing, mine[:double])
        swapped = dot(mixing, other[:double])
        net_out[w * scen : (w + 1) * scen, :half] = own
        net_out[w * scen : (w + 1) * scen, half:] = swapped
        for out in {0: (low_out, edge_out), SPAN - 1: (high_out,)}.get(w, ()):
            out[:, :half] = own
            out[:, half:] = swapped


def sum_hot(x, hot, back=False):
    product = dot if back else dot_t
    high, mid, low = three_parts(x)
    return product(high, hot) + product(mid, hot) + product(low, hot)


def sets_kernel(
    net, above, below, start, mine, other, corr, fund, limits, where, money, side_of, out
):
    scen, factors = above.shape
    half = factors // 2
    double = mine.shape[0] - 3 * half - 32
    last = (SPAN - 1) * scen
    before = above[...]
    after = below[...] + start[...]
    netted = jnp.concatenate([net[:scen] + before, net[scen:last], net[last:] + after], axis=0)
    base = double + 3 * half

    def risk_of(ref):
        return from_parts(ref[base : base + 1], ref[base + 8 : base + 9], ref[base + 16 : base + 17])

    def bucket_of(ref):
        return ref[base + 24 : base + 25].astype(F32)

    risk = jnp.concatenate([risk_of(mine), risk_of(other)], axis=1)
    bucket = jnp.concatenate([bucket_of(mine), bucket_of(other)], axis=1).astype(jnp.int32)
    hot = jnp.where(
        lax.broadcasted_iota(jnp.int32, (16, factors), 0) == bucket, 1.0, 0.0
    ).astype(BF16)
    limit = limits[:1, :16]
    bucket_sum = sum_hot(netted, hot)
    raw_ratio = jnp.sqrt(jnp.abs(bucket_sum) / limit)
    concentration = jnp.maximum(1.0, raw_ratio)
    conc_factor = sum_hot(concentration, hot, back=True)
    scaled = risk * conc_factor
    weighted = scaled * netted
    far_cols = from_parts(*[other[double + i * half : double + (i + 1) * half] for i in range(3)])
    far_rows = jnp.concatenate([corr[half:, :half], far_cols], axis=1)
    image = dot(weighted[:, :half], corr[:half], precision=PRECISE) + dot(
        weighted[:, half:], far_rows, precision=PRECISE
    )
    margin = jnp.sqrt(jnp.sum(weighted * image, axis=1, keepdims=True) + 1e-06)
    first = lax.axis_index("trades") * NSET_DEV - 1
    costs = fund[...]
    lanes = lax.broadcasted_iota(jnp.int32, costs.shape, 1)
    cost = jnp.concatenate(
        [
            jnp.sum(jnp.where(lanes == first + w, costs, 0.0), axis=1, keepdims=True)
            for w in range(SPAN)
        ],
        axis=0,
    )
    weighted_bar = (cost / margin) * image
    conc_bar = sum_hot(weighted_bar * risk * netted, hot)
    sign = jnp.where(bucket_sum > 0.0, 1.0, jnp.where(bucket_sum < 0.0, -1.0, 0.0))
    bucket_bar = jnp.where(raw_ratio > 1.0, conc_bar * sign / (2.0 * limit * concentration), 0.0)
    bar = (weighted_bar * scaled + sum_hot(bucket_bar, hot, back=True)).astype(BF16)
    grad = weighted_bar[scen:, :half] * netted[scen:, :half] * conc_factor[scen:, :half]
    weight = jnp.broadcast_to(jnp.sum(grad, axis=0, keepdims=True), (8, half)).astype(BF16)
    trades = side_of.shape[0]
    place = where[:1]
    spread = dot_t(bar[:, :half], mine[:double]) + dot_t(bar[:, half:], other[:double])
    pulled = jnp.zeros((scen, double), F32)
    for w in range(SPAN):
        pulled = pulled + jnp.where(place == w, spread[w * scen : (w + 1) * scen], 0.0)
    likely = lax.logistic(money[...])
    money_bar = (pulled[:, :trades] * likely * (1.0 - likely) + pulled[:, trades:]).astype(BF16)
    state = dot(money_bar, side_of[...]).astype(BF16)
    for i in range(out.shape[0]):
        out[i, :scen] = state
        out[i, scen:] = weight


def fold_kernel(got, total_out):
    count, rows, half = got.shape
    cols = count // NEAR
    scen = rows - 8
    mine = lax.axis_index("scen")
    state = jnp.zeros((scen, half), F32)
    for j in range(NEAR):
        state = state + got[j * cols + mine, :scen].astype(F32)
    weight = jnp.zeros((8, half), F32)
    for i in range(count):
        weight = weight + got[i, scen:].astype(F32)
    total_out[:scen] = state
    total_out[scen:] = weight


def last_kernel(count, whole, first, second, third, fourth, fifth, state_out, weight_out):
    scen = state_out.shape[0]
    devs = lax.axis_size("trades")
    late = lax.rem(lax.axis_index("trades") + NEAR // 2, devs) < NEAR
    parts = [x[...].astype(F32) for x in (first, second, third, fourth, fifth)]
    total = jnp.where(late, whole[...].astype(F32), sum(parts[1:], parts[0]))
    state_out[...] = total[:scen]
    weight_out[...] = total[scen : scen + 1] * (1.0 / count)


def near_vmem(x):
    return pltpu.with_memory_space_constraint(x, pltpu.VMEM)


def call(body, out_shape, *args, smem=()):
    return pl.pallas_call(
        body,
        out_shape=out_shape,
        in_specs=[
            pl.BlockSpec(memory_space=pltpu.SMEM if i in smem else pltpu.VMEM)
            for i in range(len(args))
        ],
        out_specs=jax.tree.map(lambda _: pl.BlockSpec(memory_space=pltpu.VMEM), out_shape),
    )(*args)


def shifted(x, axis, by, first=0):
    size = lax.axis_size(axis)
    pairs = [(i, i + by) for i in range(first, size) if 0 <= i + by < size]
    return lax.ppermute(x, axis, pairs)


def sum_over_trades(copies):
    devs, cols = lax.axis_size("trades"), lax.axis_size("scen")
    blocks = devs // NEAR
    place = lambda b, j: (b * NEAR + j - NEAR // 2) % devs
    mine = lax.rem(lax.axis_index("trades") + NEAR // 2, devs) // NEAR
    groups = [
        [place(b, j) * cols + c for j in range(NEAR) for c in range(cols)] for b in range(blocks)
    ]
    got = lax.all_to_all(copies, ("trades", "scen"), 0, 0, tiled=True, axis_index_groups=groups)
    total = call(fold_kernel, pltpu.VMEM(copies.shape[1:], F32), near_vmem(got))

    def send(x, *links):
        pairs = []
        for a, b, flip in links:
            pairs += [(place(a, NEAR - 1 - j if flip else j), place(b, j)) for j in range(NEAR)]
        return lax.ppermute(x.astype(BF16), "trades", pairs)

    far = send(total, (5, 1, 0))
    total = total + send(total, (6, 7, 0), (4, 3, 0), (2, 1, 0)).astype(F32)
    one = send(total, (7, 0, 0))
    near = send(total, (3, 1, 0))
    added = total + far.astype(F32) + near.astype(F32)
    two = send(added, (1, 0, 0))
    whole = (total + one.astype(F32) + two.astype(F32)).astype(BF16)
    first = send(whole, (0, 1, 1))
    second = send(whole, (0, 2, 1))
    third = send(first, (1, 3, 0))
    fourth = send(jnp.where(mine == 2, second, third), (3, 4, 0), (2, 5, 0))
    fifth = send(fourth, (4, 7, 0), (5, 6, 0))
    return whole, first, second, third, fourth, fifth


def on_device(
    scenario_state,
    direction,
    trade_load,
    trade_curve,
    trade_set,
    factor_bucket_index,
    threshold,
    factor_risk_weight,
    correlation,
    funding,
):
    scen, set_count = funding.shape
    trades, half = trade_load.shape
    double, factors = 2 * trades, 2 * half
    mine = call(
        pack_kernel,
        pltpu.VMEM((double + 3 * half + 32, half), BF16),
        trade_load, trade_curve, correlation,
        factor_risk_weight.reshape(1, half), factor_bucket_index.reshape(1, half),
    )
    other = lax.ppermute(mine, "fact", [(0, 1), (1, 0)])
    money, pair, side, corr, where, fund, limit = call(
        money_kernel,
        (
            pltpu.VMEM((scen, trades), F32),
            pltpu.VMEM((scen, double), BF16),
            pltpu.VMEM((trades, half), BF16),
            pltpu.VMEM((factors, factors), F32),
            pltpu.VMEM((8, double), jnp.int32),
            pltpu.VMEM(funding.shape, F32),
            pltpu.VMEM((8, 128), F32),
        ),
        near_vmem(scenario_state), near_vmem(direction), near_vmem(correlation),
        near_vmem(trade_set.reshape(1, trades)), near_vmem(funding), threshold,
        smem=(5,),
    )
    mine, other = near_vmem(mine), near_vmem(other)
    money, pair, side, corr, where, fund, limit = map(
        near_vmem, (money, pair, side, corr, where, fund, limit)
    )
    net, low, high, edge = call(
        window_kernel,
        (
            pltpu.VMEM((SPAN * scen, factors), F32),
            pltpu.VMEM((scen, factors), F32),
            pltpu.VMEM((scen, factors), F32),
            pltpu.VMEM((scen, factors), F32),
        ),
        pair, where, mine, other,
    )
    below, above, start = lax.optimization_barrier(
        (shifted(low, "trades", -1, 2), shifted(high, "trades", 1), lax.ppermute(edge, "trades", [(1, 0)]))
    )
    below, above, start = near_vmem(below), near_vmem(above), near_vmem(start)
    copies = call(
        sets_kernel,
        pltpu.VMEM((NEAR * lax.axis_size("scen"), scen + 8, half), BF16),
        near_vmem(net), above, below, start, mine, other, corr, fund, limit, where, money, side,
    )
    count = scen * lax.axis_size("scen") * set_count
    state_grad, weight_grad = call(
        functools.partial(last_kernel, count),
        (jax.ShapeDtypeStruct((scen, half), F32), jax.ShapeDtypeStruct((1, half), F32)),
        *map(near_vmem, sum_over_trades(copies)),
    )
    return (state_grad, weight_grad.reshape(half))


def solution(mesh):
    placed = (
        P(("groups", "scen"), None),
        P("trades", None),
        P("trades", "fact"),
        P("trades", "fact"),
        P("trades"),
        P("fact"),
        P(),
        P("fact"),
        P(None, "fact"),
        P(("groups", "scen"), None),
    )
    return jax.shard_map(
        on_device,
        mesh=mesh,
        in_specs=placed,
        out_specs=(P(("groups", "scen"), "fact"), P(("groups", "fact"))),
        check_vma=False,
    )
```

```python
import functools

import jax
import jax.numpy as jnp
from jax import lax
from jax.experimental import pallas as pl
from jax.experimental.pallas import tpu as pltpu
from jax.sharding import PartitionSpec as P

NSET_DEV = 4
SPAN = NSET_DEV + 1
NEAR = 4
MIRROR = (3, 2, 1, 0)
F32 = jnp.float32
BF16 = jnp.bfloat16
PRECISE = lax.Precision.HIGHEST


def three_parts(x):
    high = x.astype(BF16)
    rest = x - high.astype(F32)
    mid = rest.astype(BF16)
    low = (rest - mid.astype(F32)).astype(BF16)
    return high, mid, low


def from_parts(high, mid, low):
    return high.astype(F32) + mid.astype(F32) + low.astype(F32)


def dot_t(a, b, **kw):
    return lax.dot_general(a, b, (((1,), (1,)), ((), ())), preferred_element_type=F32, **kw)


def dot(a, b, **kw):
    return lax.dot_general(a, b, (((1,), (0,)), ((), ())), preferred_element_type=F32, **kw)


def pack_kernel(load, curve, corr, risk, bucket, out):
    trades, half = load.shape
    start = pl.multiple_of(lax.axis_index("fact") * half, half)
    out[:trades] = load[...]
    out[trades : 2 * trades] = curve[...]
    for i, part in enumerate(three_parts(corr[pl.ds(start, half)])):
        out[2 * trades + i * half : 2 * trades + (i + 1) * half] = part
    base = 2 * trades + 3 * half
    high, mid, low = three_parts(risk[...])
    for i, row in enumerate((high, mid, low, bucket[...].astype(F32).astype(BF16))):
        out[base + 8 * i : base + 8 * (i + 1)] = jnp.broadcast_to(row, (8, half))


def money_kernel(
    state, direction, corr, sets, funding, threshold,
    money_out, pair_out, side_out, corr_out, where_out, fund_out, limit_out,
):
    money = dot_t(state[...], direction[...])
    money_out[...] = money
    trades, factors = direction.shape
    half = factors // 2
    pair_out[:, :trades] = lax.logistic(money).astype(BF16)
    pair_out[:, trades:] = money.astype(BF16)
    side = pl.multiple_of(lax.axis_index("fact") * half, half)
    side_out[...] = direction[:, pl.ds(side, half)]
    far_side = pl.multiple_of((1 - lax.axis_index("fact")) * half, half)
    cross = corr[pl.ds(far_side, half)]
    corr_out[:half, :half] = corr[pl.ds(side, half)]
    corr_out[half:, :half] = cross
    corr_out[:half, half:] = cross.T
    first = lax.axis_index("trades") * NSET_DEV - 1
    place = jnp.broadcast_to(sets[...] - first, (8, trades))
    where_out[:, :trades] = place
    where_out[:, trades:] = place
    fund_out[...] = funding[...]
    buckets = lax.broadcasted_iota(jnp.int32, limit_out.shape, 1)
    limit = jnp.ones(limit_out.shape, F32)
    for i in range(threshold.shape[0]):
        limit = jnp.where(buckets == i, threshold[i], limit)
    limit_out[...] = limit


def window_kernel(pair, where, mine, other, net_out, low_out, high_out, edge_out):
    scen, double = pair.shape
    paired = pair[...]
    place = where[:1]
    half = mine.shape[1]
    for w in range(SPAN):
        member = jnp.where(place == w, 1.0, 0.0).astype(BF16)
        mixing = paired * member
        own = dot(mixing, mine[:double])
        swapped = dot(mixing, other[:double])
        net_out[w * scen : (w + 1) * scen, :half] = own
        net_out[w * scen : (w + 1) * scen, half:] = swapped
        for out in {0: (low_out, edge_out), SPAN - 1: (high_out,)}.get(w, ()):
            out[:, :half] = own
            out[:, half:] = swapped


def sum_hot(x, hot, back=False):
    product = dot if back else dot_t
    high, mid, low = three_parts(x)
    return product(high, hot) + product(mid, hot) + product(low, hot)


def sets_kernel(
    net, above, below, start, mine, other, corr, fund, limits, where, money, side_of, out
):
    scen, factors = above.shape
    half = factors // 2
    double = mine.shape[0] - 3 * half - 32
    last = (SPAN - 1) * scen
    before = above[...]
    after = below[...] + start[...]
    netted = jnp.concatenate([net[:scen] + before, net[scen:last], net[last:] + after], axis=0)
    base = double + 3 * half

    def risk_of(ref):
        return from_parts(ref[base : base + 1], ref[base + 8 : base + 9], ref[base + 16 : base + 17])

    def bucket_of(ref):
        return ref[base + 24 : base + 25].astype(F32)

    risk = jnp.concatenate([risk_of(mine), risk_of(other)], axis=1)
    bucket = jnp.concatenate([bucket_of(mine), bucket_of(other)], axis=1).astype(jnp.int32)
    hot = jnp.where(
        lax.broadcasted_iota(jnp.int32, (16, factors), 0) == bucket, 1.0, 0.0
    ).astype(BF16)
    limit = limits[:1, :16]
    bucket_sum = sum_hot(netted, hot)
    raw_ratio = jnp.sqrt(jnp.abs(bucket_sum) / limit)
    concentration = jnp.maximum(1.0, raw_ratio)
    conc_factor = sum_hot(concentration, hot, back=True)
    scaled = risk * conc_factor
    weighted = scaled * netted
    far_cols = from_parts(*[other[double + i * half : double + (i + 1) * half] for i in range(3)])
    far_rows = jnp.concatenate([corr[half:, :half], far_cols], axis=1)
    image = dot(weighted[:, :half], corr[:half], precision=PRECISE) + dot(
        weighted[:, half:], far_rows, precision=PRECISE
    )
    margin = jnp.sqrt(jnp.sum(weighted * image, axis=1, keepdims=True) + 1e-06)
    first = lax.axis_index("trades") * NSET_DEV - 1
    costs = fund[...]
    lanes = lax.broadcasted_iota(jnp.int32, costs.shape, 1)
    cost = jnp.concatenate(
        [
            jnp.sum(jnp.where(lanes == first + w, costs, 0.0), axis=1, keepdims=True)
            for w in range(SPAN)
        ],
        axis=0,
    )
    weighted_bar = (cost / margin) * image
    conc_bar = sum_hot(weighted_bar * risk * netted, hot)
    sign = jnp.where(bucket_sum > 0.0, 1.0, jnp.where(bucket_sum < 0.0, -1.0, 0.0))
    bucket_bar = jnp.where(raw_ratio > 1.0, conc_bar * sign / (2.0 * limit * concentration), 0.0)
    bar = (weighted_bar * scaled + sum_hot(bucket_bar, hot, back=True)).astype(BF16)
    grad = weighted_bar[scen:, :half] * netted[scen:, :half] * conc_factor[scen:, :half]
    weight = jnp.broadcast_to(jnp.sum(grad, axis=0, keepdims=True), (8, half)).astype(BF16)
    trades = side_of.shape[0]
    place = where[:1]
    spread = dot_t(bar[:, :half], mine[:double]) + dot_t(bar[:, half:], other[:double])
    pulled = jnp.zeros((scen, double), F32)
    for w in range(SPAN):
        pulled = pulled + jnp.where(place == w, spread[w * scen : (w + 1) * scen], 0.0)
    likely = lax.logistic(money[...])
    money_bar = (pulled[:, :trades] * likely * (1.0 - likely) + pulled[:, trades:]).astype(BF16)
    state = dot(money_bar, side_of[...]).astype(BF16)
    for i in range(out.shape[0]):
        out[i, :scen] = state
        out[i, scen:] = weight


def fold_kernel(got, total_out):
    count, rows, half = got.shape
    cols = count // NEAR
    scen = rows - 8
    mine = lax.axis_index("scen")
    state = jnp.zeros((scen, half), F32)
    for j in range(NEAR):
        state = state + got[j * cols + mine, :scen].astype(F32)
    weight = jnp.zeros((8, half), F32)
    for i in range(count):
        weight = weight + got[i, scen:].astype(F32)
    total_out[:scen] = state
    total_out[scen:] = weight


def last_kernel(count, whole, first, second, third, fourth, fifth, state_out, weight_out):
    scen = state_out.shape[0]
    devs = lax.axis_size("trades")
    late = lax.rem(lax.axis_index("trades") + NEAR // 2, devs) < NEAR
    parts = [x[...].astype(F32) for x in (first, second, third, fourth, fifth)]
    total = jnp.where(late, whole[...].astype(F32), sum(parts[1:], parts[0]))
    state_out[...] = total[:scen]
    weight_out[...] = total[scen : scen + 1] * (1.0 / count)


def near_vmem(x):
    return pltpu.with_memory_space_constraint(x, pltpu.VMEM)


def call(body, out_shape, *args, smem=()):
    return pl.pallas_call(
        body,
        out_shape=out_shape,
        in_specs=[
            pl.BlockSpec(memory_space=pltpu.SMEM if i in smem else pltpu.VMEM)
            for i in range(len(args))
        ],
        out_specs=jax.tree.map(lambda _: pl.BlockSpec(memory_space=pltpu.VMEM), out_shape),
    )(*args)


def shifted(x, axis, by, first=0):
    size = lax.axis_size(axis)
    pairs = [(i, i + by) for i in range(first, size) if 0 <= i + by < size]
    return lax.ppermute(x, axis, pairs)


def sum_over_trades(copies):
    devs, cols = lax.axis_size("trades"), lax.axis_size("scen")
    blocks = devs // NEAR
    place = lambda b, j: (b * NEAR + j - NEAR // 2) % devs
    mine = lax.rem(lax.axis_index("trades") + NEAR // 2, devs) // NEAR
    groups = [
        [place(b, j) * cols + c for j in range(NEAR) for c in range(cols)] for b in range(blocks)
    ]
    got = lax.all_to_all(copies, ("trades", "scen"), 0, 0, tiled=True, axis_index_groups=groups)
    total = call(fold_kernel, pltpu.VMEM(copies.shape[1:], F32), near_vmem(got))

    def send(x, *links):
        pairs = []
        for a, b, flip in links:
            order = flip or range(NEAR)
            pairs += [(place(a, order[j]), place(b, j)) for j in range(NEAR)]
        return lax.ppermute(x.astype(BF16), "trades", pairs)

    far = send(total, (5, 1, 0))
    total = total + send(total, (6, 7, 0), (4, 3, 0), (2, 1, 0)).astype(F32)
    one = send(total, (7, 0, (0, 1, 3, 2)))
    near = send(total, (3, 1, 0))
    added = total + far.astype(F32) + near.astype(F32)
    two = send(added, (1, 0, (0, 2, 1, 3)))
    whole = (total + one.astype(F32) + two.astype(F32)).astype(BF16)
    first = send(whole, (0, 1, MIRROR))
    second = send(whole, (0, 2, MIRROR))
    third = send(first, (1, 3, 0))
    fourth = send(jnp.where(mine == 2, second, third), (3, 4, 0), (2, 5, 0))
    fifth = send(fourth, (4, 7, 0), (5, 6, 0))
    return whole, first, second, third, fourth, fifth


def on_device(
    scenario_state,
    direction,
    trade_load,
    trade_curve,
    trade_set,
    factor_bucket_index,
    threshold,
    factor_risk_weight,
    correlation,
    funding,
):
    scen, set_count = funding.shape
    trades, half = trade_load.shape
    double, factors = 2 * trades, 2 * half
    mine = call(
        pack_kernel,
        pltpu.VMEM((double + 3 * half + 32, half), BF16),
        trade_load, trade_curve, correlation,
        factor_risk_weight.reshape(1, half), factor_bucket_index.reshape(1, half),
    )
    other = lax.ppermute(mine, "fact", [(0, 1), (1, 0)])
    money, pair, side, corr, where, fund, limit = call(
        money_kernel,
        (
            pltpu.VMEM((scen, trades), F32),
            pltpu.VMEM((scen, double), BF16),
            pltpu.VMEM((trades, half), BF16),
            pltpu.VMEM((factors, factors), F32),
            pltpu.VMEM((8, double), jnp.int32),
            pltpu.VMEM(funding.shape, F32),
            pltpu.VMEM((8, 128), F32),
        ),
        near_vmem(scenario_state), near_vmem(direction), near_vmem(correlation),
        near_vmem(trade_set.reshape(1, trades)), near_vmem(funding), threshold,
        smem=(5,),
    )
    mine, other = near_vmem(mine), near_vmem(other)
    money, pair, side, corr, where, fund, limit = map(
        near_vmem, (money, pair, side, corr, where, fund, limit)
    )
    net, low, high, edge = call(
        window_kernel,
        (
            pltpu.VMEM((SPAN * scen, factors), F32),
            pltpu.VMEM((scen, factors), F32),
            pltpu.VMEM((scen, factors), F32),
            pltpu.VMEM((scen, factors), F32),
        ),
        pair, where, mine, other,
    )
    below, above, start = lax.optimization_barrier(
        (shifted(low, "trades", -1, 2), shifted(high, "trades", 1), lax.ppermute(edge, "trades", [(1, 0)]))
    )
    below, above, start = near_vmem(below), near_vmem(above), near_vmem(start)
    copies = call(
        sets_kernel,
        pltpu.VMEM((NEAR * lax.axis_size("scen"), scen + 8, half), BF16),
        near_vmem(net), above, below, start, mine, other, corr, fund, limit, where, money, side,
    )
    count = scen * lax.axis_size("scen") * set_count
    state_grad, weight_grad = call(
        functools.partial(last_kernel, count),
        (jax.ShapeDtypeStruct((scen, half), F32), jax.ShapeDtypeStruct((1, half), F32)),
        *map(near_vmem, sum_over_trades(copies)),
    )
    return (state_grad, weight_grad.reshape(half))


def solution(mesh):
    placed = (
        P(("groups", "scen"), None),
        P("trades", None),
        P("trades", "fact"),
        P("trades", "fact"),
        P("trades"),
        P("fact"),
        P(),
        P("fact"),
        P(None, "fact"),
        P(("groups", "scen"), None),
    )
    return jax.shard_map(
        on_device,
        mesh=mesh,
        in_specs=placed,
        out_specs=(P(("groups", "scen"), "fact"), P(("groups", "fact"))),
        check_vma=False,
    )
```
